32 devices in a mesh: crop: 4 (over x, core), row: 8 (over z, y).
Axes of the slice: x: 2, y: 2, z: 4, core: 2. Of those that a mesh axis runs over, the one named last changes fastest.
Arguments:
- pair: float32 [768, 192, 128], P(('crop', 'row')), parts along dimension 0, may hold values from -6 to 6
- single: float32 [768, 384], P(('crop', 'row')), parts along dimension 0, may hold values from -6 to 6
- token_mask: int32 [768], P('crop'), parts along dimension 0, may hold values from 0 to 1, as said below
- w_tri_proj: bfloat16 [128, 512], replicated, may hold values from -0.5 to 0.5
- w_tri_gate: bfloat16 [128, 128], replicated, may hold values from -0.5 to 0.5
- w_tri_out: bfloat16 [128, 128], replicated, may hold values from -0.5 to 0.5
- w_trans_in: bfloat16 [128, 1024], replicated, may hold values from -0.5 to 0.5
- w_trans_out: bfloat16 [512, 128], replicated, may hold values from -0.25 to 0.25
- w_bias: bfloat16 [128, 16], replicated, may hold values from -0.5 to 0.5
- w_query: bfloat16 [384, 384], replicated, may hold values from -16 to 16
- w_key: bfloat16 [384, 384], replicated, may hold values from -0.5 to 0.5
- w_value_gate: bfloat16 [384, 768], replicated, may hold values from -0.3125 to 0.3125
- w_out: bfloat16 [384, 384], replicated, may hold values from -0.3125 to 0.3125
Outputs:
- pair_new: float32 [768, 192, 128], P(('crop', 'row')), parts along dimension 0
- single_update: float32 [768, 384], P(('crop', 'row')), parts along dimension 0
The draws below stay inside these ranges and needn't reach their ends.
There are 4 independent parts, one for each index of `crop`. The reference program is written for one: setup_inputs(seed, part) draws one part's arguments, and reference() takes and returns one part's arrays. A program takes and returns all parts, laid end to end along the dimension named above; an argument that names none is the same for every part. Nothing has to cross between parts.
Inputs may be any that keep to these rules, and one draw needn't show every extreme that they name: `token_mask`: ones for the first tokens of a crop and zeros after them; at least 96 ones.
All inputs are finite; a program needn't handle non-finite values.
Results may differ from the reference program's by a relative error of at most 0.013.
The reference program's roundings to bfloat16 on the way (of `normed`, `triangle_normed`, `inner_act`, `probs` and `gated`) count: a program that leaves them out, or rounds other values in their place, can miss the bound.
Values may be sent and summed in bfloat16 or wider, within the bound.
No kernel may reach another device: no remote copies, remote signals or barrier semaphores. Data moves between devices by JAX's collectives and lax.ppermute only.
A program may use at most 128 MiB of HBM per device.

```python
import math
import jax
import jax.numpy as jnp
from jax import lax

C = 128
CH = 128
CS = 384
HEADS = 16
FF = 512
N = 192


def query_key_pair(key):
    base_weight = jnp.clip(jax.random.normal(jax.random.fold_in(key, 7101), (CS, CS), jnp.float32) * CS ** (-0.5), -0.5, 0.5)
    noise_weight = jnp.clip(jax.random.normal(jax.random.fold_in(key, 7102), (CS, CS), jnp.float32) * CS ** (-0.5), -0.5, 0.5)
    query_weight = noise_weight
    return (query_weight, base_weight)


def draw_w_query(key, part):
    return query_key_pair(key)[0].astype(jnp.bfloat16)


def draw_w_key(key, part):
    return query_key_pair(key)[1].astype(jnp.bfloat16)


def draw_token_mask(key, part):
    count = jax.random.randint(jax.random.fold_in(key, 7201), (), N // 2, N + 1)
    positions = jnp.arange(N, dtype=jnp.int32)
    return (positions < count).astype(jnp.int32)


def levels(key, shape, split, smallest, largest):
    gain = 1.0
    for position, parts in split:
        heights = jax.random.uniform(jax.random.fold_in(jax.random.fold_in(key, 6), position), (parts,), jnp.float32, smallest / len(split), largest / len(split))
        gain = gain * jnp.repeat(jnp.exp(heights), shape[position] // parts).reshape((-1,) + (1,) * (len(shape) - 1 - position))
    return gain


def centred(stream_key, extent, width, most, pieces=(), kind=jnp.bfloat16):
    gain = levels(stream_key, extent, pieces, -0.22, 0.18) if pieces else 1.0
    drawn = jax.random.normal(stream_key, extent, jnp.float32) * width * gain
    return jnp.minimum(jnp.maximum(drawn, -most), most).astype(kind)


def setup_inputs(seed: int = 0, part: int = 0) -> dict:
    keys = jax.random.split(jax.random.key(seed), 14)
    own_keys = jax.random.split(jax.random.fold_in(keys[13], part), 14)
    return {
        "pair": centred(own_keys[0], (N, N, C), 1.0, 6.0, ((0, 8),), jnp.float32),
        "single": centred(own_keys[1], (N, CS), 1.0, 6.0, ((0, 8),), jnp.float32),
        "token_mask": draw_token_mask(jax.random.fold_in(jax.random.fold_in(keys[13], part), 71), part),
        "w_tri_proj": centred(keys[3], (C, 4 * CH), C ** -0.5, 0.5),
        "w_tri_gate": centred(keys[4], (C, C), C ** -0.5, 0.5),
        "w_tri_out": centred(keys[5], (CH, C), CH ** -0.5, 0.5),
        "w_trans_in": centred(keys[6], (C, 2 * FF), C ** -0.5, 0.5),
        "w_trans_out": centred(keys[7], (FF, C), FF ** -0.5, 0.25),
        "w_bias": centred(keys[8], (C, HEADS), C ** -0.5, 0.5),
        "w_query": draw_w_query(jax.random.fold_in(keys[13], 71), part),
        "w_key": draw_w_key(jax.random.fold_in(keys[13], 71), part),
        "w_value_gate": centred(keys[11], (CS, 2 * CS), CS ** -0.5, 0.3125),
        "w_out": centred(keys[12], (CS, CS), CS ** -0.5, 0.3125),
    }


epsilon = 1e-05

def layer_norm(values_in, along):
    average = lax.optimization_barrier(jnp.mean(values_in, axis=along, keepdims=True))
    centered = values_in - average
    spread = lax.optimization_barrier(jnp.mean(centered * centered, axis=along, keepdims=True))
    return centered * lax.rsqrt(spread + epsilon)

def reference(pair, single, token_mask, w_tri_proj, w_tri_gate, w_tri_out, w_trans_in, w_trans_out, w_bias, w_query, w_key, w_value_gate, w_out):
    length = pair.shape[0]
    pair_width = pair.shape[2]
    hidden = w_tri_out.shape[0]
    inner_width = w_trans_out.shape[0]
    head_count = w_bias.shape[1]
    channels = single.shape[1]
    head_size = channels // head_count
    live_all = token_mask.astype(jnp.float32)
    pair_live = live_all[:, None] * live_all[None, :]
    block_rows = math.gcd(length, 8)
    block_count = length // block_rows

    def project(inputs):
        row_slab, slab_live = inputs
        normed = layer_norm(row_slab, 2).astype(jnp.bfloat16).reshape(-1, pair_width)
        projected = jnp.dot(normed, w_tri_proj, preferred_element_type=jnp.float32).reshape(block_rows, length, 4, hidden)
        left_edge = (jax.nn.sigmoid(projected[:, :, 1]) * projected[:, :, 0] * slab_live[:, :, None]).astype(jnp.bfloat16)
        right_edge = (jax.nn.sigmoid(projected[:, :, 3]) * projected[:, :, 2] * slab_live[:, :, None]).astype(jnp.bfloat16)
        gate_pair = jax.nn.sigmoid(jnp.dot(normed, w_tri_gate, preferred_element_type=jnp.float32)).reshape(block_rows, length, pair_width)
        return (left_edge, right_edge, gate_pair)
    left_edge, right_edge, gate_pair = lax.map(project, (pair.reshape(block_count, block_rows, length, pair_width), pair_live.reshape(block_count, block_rows, length)))
    left_edge = jnp.transpose(left_edge.reshape(length, length, hidden), (2, 0, 1))
    right_edge = jnp.transpose(right_edge.reshape(length, length, hidden), (2, 0, 1))
    gate_pair = gate_pair.reshape(length, length, pair_width)

    def channel_product(operands):
        return jnp.dot(operands[0], operands[1].T, preferred_element_type=jnp.float32)
    triangle = lax.map(channel_product, (left_edge, right_edge))
    triangle_normed = layer_norm(triangle, 0).astype(jnp.bfloat16)
    tri_out = jnp.einsum('cij,cd->ijd', triangle_normed.astype(jnp.float32), w_tri_out.astype(jnp.float32))
    pair_mid = pair + gate_pair * tri_out

    def transition(row_slab):
        trans_normed = layer_norm(row_slab, 2).astype(jnp.bfloat16).reshape(-1, pair_width)
        gate_up = jnp.dot(trans_normed, w_trans_in, preferred_element_type=jnp.float32)
        inner_act = (jax.nn.silu(gate_up[:, :inner_width]) * gate_up[:, inner_width:]).astype(jnp.bfloat16)
        update = jnp.dot(inner_act, w_trans_out, preferred_element_type=jnp.float32)
        return row_slab + update.reshape(block_rows, length, pair_width)
    pair_new = lax.map(transition, pair_mid.reshape(block_count, block_rows, length, pair_width)).reshape(length, length, pair_width)

    def bias_rows(row_slab):
        bias_normed = layer_norm(row_slab, 2).astype(jnp.bfloat16).reshape(-1, pair_width)
        return jnp.dot(bias_normed, w_bias, preferred_element_type=jnp.float32).reshape(block_rows, length, head_count)
    bias = lax.map(bias_rows, pair_new.reshape(block_count, block_rows, length, pair_width)).reshape(length, length, head_count)
    bias = jnp.transpose(bias, (2, 0, 1))
    single_normed = layer_norm(single, 1).astype(jnp.bfloat16)
    queries = jnp.dot(single_normed, w_query, preferred_element_type=jnp.float32).astype(jnp.bfloat16)
    keys_all = jnp.dot(single_normed, w_key, preferred_element_type=jnp.float32).astype(jnp.bfloat16)
    values_all = jnp.dot(single_normed, w_value_gate[:, :channels], preferred_element_type=jnp.float32).astype(jnp.bfloat16)
    att_gate = jax.nn.sigmoid(jnp.dot(single_normed, w_value_gate[:, channels:], preferred_element_type=jnp.float32))
    query_heads = queries.astype(jnp.float32).reshape(length, head_count, head_size)
    key_heads = keys_all.astype(jnp.float32).reshape(length, head_count, head_size)
    value_heads = values_all.astype(jnp.float32).reshape(length, head_count, head_size)
    scores = jnp.einsum('ihd,jhd->hij', query_heads, key_heads) / jnp.sqrt(jnp.float32(head_size)) + bias
    scores = jnp.where(live_all[None, None, :] > 0, scores, jnp.float32(-1000000000.0))
    row_max = lax.optimization_barrier(jnp.max(scores, axis=2, keepdims=True))
    weights = jnp.exp(scores - row_max)
    weights = weights / lax.optimization_barrier(jnp.sum(weights, axis=2, keepdims=True))
    probs = weights.astype(jnp.bfloat16)
    attended = jnp.einsum('hij,jhd->ihd', probs.astype(jnp.float32), value_heads).reshape(length, channels)
    gated = (att_gate * attended).astype(jnp.bfloat16)
    single_update = jnp.dot(gated, w_out, preferred_element_type=jnp.float32)
    return (pair_new, single_update)
```

```python
import functools
import math

import jax
import jax.numpy as jnp
from jax import lax
from jax.experimental import pallas as pl
from jax.experimental.pallas import tpu as pltpu
from jax.sharding import PartitionSpec as P

epsilon = 1e-05
LANES = 128
SUB = 8
f32 = jnp.float32
bf16 = jnp.bfloat16
NT = (((1,), (1,)), ((), ()))


def layer_norm(values_in, along):
    average = jnp.mean(values_in, axis=along, keepdims=True)
    centered = values_in - average
    spread = jnp.mean(centered * centered, axis=along, keepdims=True)
    return centered * lax.rsqrt(spread + epsilon)


def sigmoid(x):
    return 0.5 * jnp.tanh(0.5 * x) + 0.5


def repeat_rest(x, full):
    return jnp.concatenate([x, x[full:]], axis=0)


def first_half_lanes(shape):
    return lax.broadcasted_iota(jnp.int32, shape, len(shape) - 1) < LANES // 2


def edges_to_messages(me_ref, mask_ref, live_ref, wt_ref, rows_of, head_ref, rest_ref, out_refs, hidden, full):
    sets = len(out_refs)
    per_set = hidden // sets
    pairs = per_set // 2
    step = pl.program_id(0)
    row_count = SUB * pl.num_programs(0)
    me = me_ref[0]
    own_set = lax.rem(me, sets)
    first = me * row_count + step * SUB
    for j in range(SUB):
        x = repeat_rest(rows_of(j), full)
        projected = lax.dot_general(wt_ref[...], x, NT, preferred_element_type=f32)
        live = live_ref[...] * mask_ref[first + j].astype(f32)
        edge = sigmoid(projected[hidden:]) * projected[:hidden] * live
        for s in range(sets):
            q = lax.bitwise_xor(own_set, s)
            at = pl.multiple_of(j * hidden + q * per_set, per_set)
            part = edge[s * per_set : (s + 1) * per_set]
            head_ref[pl.ds(at, per_set), :] = part[:, :LANES]
            rest_ref[pl.ds(at, per_set), :] = part[:, LANES:]
    low = first_half_lanes((SUB, LANES))
    for q in range(sets):
        for c in range(pairs):
            a = pl.ds(q * per_set + c, SUB, stride=hidden)
            b = pl.ds(q * per_set + pairs + c, SUB, stride=hidden)
            out_refs[q][c, 0] = head_ref[a, :].astype(bf16)
            out_refs[q][pairs + c, 0] = head_ref[b, :].astype(bf16)
            out_refs[q][per_set + c, 0] = jnp.where(low, rest_ref[a, :], rest_ref[b, :]).astype(bf16)


def right_kernel(hidden, full, sets, me_ref, mask_ref, pair_ref, single_ref, live_ref, w_ref, *rest):
    normed_ref, out_refs = rest[0], rest[1 : 1 + sets]
    head_ref, rest_ref, wt_ref = rest[1 + sets :]

    @pl.when(pl.program_id(0) == 0)
    def _():
        wt_ref[...] = w_ref[...].T

    def rows_of(j):
        x = layer_norm(pair_ref[j], 1).astype(bf16)
        normed_ref[j] = x
        return x

    edges_to_messages(me_ref, mask_ref, live_ref, wt_ref, rows_of, head_ref, rest_ref, out_refs, hidden, full)
    single_normed = layer_norm(single_ref[...], 1).astype(bf16)
    slabs = single_ref.shape[1] // LANES
    base = hidden // sets * 3 // 2
    for q in range(sets):
        for t in range(slabs):
            out_refs[q][base + t, 0] = single_normed[:, t * LANES : (t + 1) * LANES]


def left_kernel(hidden, full, sets, me_ref, mask_ref, normed_ref, live_ref, w_ref, w_gate_ref, *rest):
    gate_ref, out_refs = rest[0], rest[1 : 1 + sets]
    head_ref, rest_ref, wt_ref = rest[1 + sets :]

    @pl.when(pl.program_id(0) == 0)
    def _():
        wt_ref[...] = w_ref[...].T

    edges_to_messages(
        me_ref, mask_ref, live_ref, wt_ref, lambda j: normed_ref[j], head_ref, rest_ref, out_refs, hidden, full
    )
    for j in range(SUB):
        gate_ref[j] = sigmoid(jnp.dot(normed_ref[j], w_gate_ref[...], preferred_element_type=f32))


def plain_rows(block):
    wide = block.astype(f32)
    return wide.reshape(wide.shape[0] * wide.shape[1], wide.shape[2])


def triangle_kernel(groups, sets, per_set, full, chunks, me_ref, *refs):
    right_refs, left_refs = refs[:groups], refs[groups : groups + sets]
    out_refs = refs[groups + sets : -4]
    head_ref, rest_ref, sums_ref, sums_rest_ref = refs[-4:]
    pairs = per_set // 2
    rows = left_refs[0].shape[1] * SUB
    length = groups * rows
    me = me_ref[0]
    total = sets * rows
    low = first_half_lanes((total, LANES))

    def channel(c, carry):
        for s in range(groups):
            d = lax.bitwise_xor(me, s)
            head_ref[0, d] = plain_rows(right_refs[s][c])
            head_ref[1, d] = plain_rows(right_refs[s][pairs + c])
            rest_ref[d] = plain_rows(right_refs[s][per_set + c])
        right_rest = repeat_rest(rest_ref[...].reshape(length, LANES), full).astype(bf16)
        left_rest = jnp.concatenate([plain_rows(r[per_set + c]) for r in left_refs], axis=0)
        for p in range(2):
            right = repeat_rest(head_ref[p].reshape(length, LANES), full).astype(bf16)
            left = jnp.concatenate([plain_rows(r[p * pairs + c]) for r in left_refs], axis=0).astype(bf16)
            kept = jnp.where(low if p == 0 else jnp.logical_not(low), left_rest, 0.0).astype(bf16)
            sums = lax.dot_general(
                jnp.concatenate([left, kept], axis=1),
                jnp.concatenate([right, right_rest], axis=1),
                NT,
                preferred_element_type=f32,
            )
            at = pl.multiple_of((p * pairs + c) * total, SUB)
            sums_ref[pl.ds(at, total), :] = sums[:, :LANES]
            sums_rest_ref[pl.ds(at, total), :] = sums[:, LANES:]
        return carry

    lax.fori_loop(0, pairs, channel, 0)
    low_half = first_half_lanes((pairs, LANES))
    n = len(chunks)
    for a in range(sets):
        base = 0
        for k, size in enumerate(chunks):
            for i in range(size):
                at = pl.ds(a * rows + base + i, per_set, stride=total)
                rest = sums_rest_ref[at, :]
                out = out_refs[a * n + k]
                out[i, :per_set] = sums_ref[at, :].astype(bf16)
                out[i, per_set:] = jnp.where(low_half, rest[:pairs], rest[pairs:]).astype(bf16)
            base += size


def attention_in_kernel(groups, me_ref, *refs):
    right_refs = refs[:groups]
    w_query_ref, w_key_ref, w_value_gate_ref, q_ref, k_ref, v_ref, g_ref, all_ref = refs[groups:]
    channels = w_query_ref.shape[0]
    me = me_ref[0]
    for s in range(groups):
        d = lax.bitwise_xor(me, s)
        for t in range(channels // LANES):
            all_ref[d, :, t * LANES : (t + 1) * LANES] = plain_rows(right_refs[s][t])
    own = all_ref[me].astype(bf16)
    every = all_ref[...].reshape(k_ref.shape).astype(bf16)
    q_ref[...] = jnp.dot(own, w_query_ref[...], preferred_element_type=f32).astype(bf16)
    g_ref[...] = sigmoid(jnp.dot(own, w_value_gate_ref[:, channels:], preferred_element_type=f32))
    k_ref[...] = jnp.dot(every, w_key_ref[...], preferred_element_type=f32).astype(bf16)
    v_ref[...] = jnp.dot(every, w_value_gate_ref[:, :channels], preferred_element_type=f32).astype(bf16)


def tail_kernel(sets, per_set, heads, me_ref, *refs):
    tri_refs = refs[:sets]
    (pair_ref, gate_ref, w_tri_out_ref, w_in_ref, w_down_ref, w_bias_ref, q_ref, k_ref, v_ref, g_ref, live_ref, w_out_ref) = refs[sets : sets + 12]
    new_ref, single_ref, w_rel_ref, wb_ref, bias_ref = refs[-5:]
    pairs = per_set // 2
    length, width = pair_ref.shape[1:]
    inner_width = w_down_ref.shape[0]
    channels = w_out_ref.shape[0]
    head_size = channels // heads
    me = me_ref[0]

    @pl.when(pl.program_id(0) == 0)
    def _():
        own_set = lax.rem(me, sets)
        for a in range(sets):
            w_rel_ref[a * per_set : (a + 1) * per_set] = w_tri_out_ref[lax.bitwise_xor(own_set, a)]
        wb_ref[...] = w_bias_ref[...].T

    def row(i, carry):
        head, rest = [], []
        for r in tri_refs:
            block = r[i].astype(f32)
            head.append(block[:per_set])
            packed = block[per_set:]
            rest.append(packed)
            rest.append(pltpu.roll(packed, LANES // 2, 1))
        tri = jnp.concatenate([jnp.concatenate(head, axis=0), jnp.concatenate(rest, axis=0)], axis=1)
        tri = layer_norm(tri, 0).astype(bf16).T[:length]
        tri_out = jnp.dot(tri, w_rel_ref[...], preferred_element_type=f32)
        mid = pair_ref[i] + gate_ref[i] * tri_out
        trans = layer_norm(mid, 1).astype(bf16)
        gate_up = jnp.dot(trans, w_in_ref[...], preferred_element_type=f32)
        gate = gate_up[:, :inner_width]
        inner = (gate * sigmoid(gate) * gate_up[:, inner_width:]).astype(bf16)
        new = mid + jnp.dot(inner, w_down_ref[...], preferred_element_type=f32)
        new_ref[i] = new
        normed = layer_norm(new, 1).astype(bf16)
        at = pl.multiple_of(i * heads, heads)
        bias_ref[pl.ds(at, heads), :] = lax.dot_general(wb_ref[...], normed, NT, preferred_element_type=f32)
        return carry

    lax.fori_loop(0, SUB, row, 0)
    wide = q_ref[...].astype(f32)
    of_head = lax.broadcasted_iota(jnp.int32, (SUB, heads, channels), 1)
    lane = lax.broadcasted_iota(jnp.int32, (SUB, heads, channels), 2)
    mine = jnp.logical_and(lane >= of_head * head_size, lane < (of_head + 1) * head_size)
    spread = jnp.where(mine, jnp.broadcast_to(wide[:, None, :], mine.shape), 0.0)
    spread = spread.reshape(SUB * heads, channels).astype(bf16)
    scores = lax.dot_general(spread, k_ref[...], NT, preferred_element_type=f32)
    scores = scores / jnp.sqrt(f32(head_size)) + bias_ref[...]
    scores = jnp.where(live_ref[...] > 0, scores, f32(-1000000000.0))
    weights = jnp.exp(scores - jnp.max(scores, axis=1, keepdims=True))
    weights = weights / jnp.sum(weights, axis=1, keepdims=True)
    attended = jnp.dot(weights.astype(bf16), v_ref[...], preferred_element_type=f32)
    attended = jnp.sum(jnp.where(mine, attended.reshape(mine.shape), 0.0), axis=1)
    gated = (g_ref[...] * attended).astype(bf16)
    single_ref[...] = jnp.dot(gated, w_out_ref[...], preferred_element_type=f32)


def whole_block(shape):
    return pl.BlockSpec(shape, lambda *_: (0,) * len(shape))


def params():
    return pltpu.CompilerParams(dimension_semantics=("arbitrary",))


def exchange(x, groups, s):
    return x if s == 0 else lax.ppermute(x, "row", [(r, r ^ s) for r in range(groups)])


def fast_body(
    pair, single, token_mask, w_tri_proj, w_tri_gate, w_tri_out, w_trans_in, w_trans_out, w_bias, w_query, w_key, w_value_gate, w_out
):
    row_count, length, width = pair.shape
    groups = lax.axis_size("row")
    sets = groups // 2
    hidden = w_tri_out.shape[0]
    per_set = hidden // sets
    message = per_set * 3 // 2
    inner_width = w_trans_out.shape[0]
    heads = w_bias.shape[1]
    channels = single.shape[1]
    slabs = channels // LANES
    full = length // LANES * LANES
    lanes = full + LANES
    tiles = row_count // SUB
    me = lax.axis_index("row").astype(jnp.int32).reshape(1)
    live = token_mask.astype(f32)
    live_lanes = repeat_rest(live, full).reshape(1, lanes)
    grid = (tiles,)
    row_block = lambda *shape: pl.BlockSpec((SUB,) + shape, lambda g, *_: (g,) + (0,) * len(shape))
    message_block = lambda n: pl.BlockSpec((n, 1, SUB, LANES), lambda g, *_: (0, g, 0, 0))
    sds = jax.ShapeDtypeStruct
    edge_scratch = [pltpu.VMEM((SUB * hidden, LANES), f32)] * 2 + [pltpu.VMEM((2 * hidden, width), bf16)]
    edge_flops = 2 * row_count * lanes * width * 2 * hidden

    normed, *right = pl.pallas_call(
        functools.partial(right_kernel, hidden, full, sets),
        name="right",
        grid_spec=pltpu.PrefetchScalarGridSpec(
            num_scalar_prefetch=2,
            grid=grid,
            in_specs=[
                row_block(length, width),
                row_block(channels),
                whole_block((1, lanes)),
                pl.BlockSpec((width, 2 * hidden), lambda *_: (0, 1)),
            ],
            out_specs=[row_block(length, width)] + [message_block(message + slabs)] * sets,
            scratch_shapes=edge_scratch,
        ),
        out_shape=[sds(pair.shape, bf16)] + [sds((message + slabs, tiles, SUB, LANES), bf16)] * sets,
        compiler_params=params(),
        cost_estimate=pl.CostEstimate(flops=edge_flops, bytes_accessed=6000000, transcendentals=0),
    )(me, token_mask, pair, single, live_lanes, w_tri_proj)

    right_in = [exchange(right[s % sets], groups, s) for s in range(groups)]

    gate_pair, *left = pl.pallas_call(
        functools.partial(left_kernel, hidden, full, sets),
        name="left",
        grid_spec=pltpu.PrefetchScalarGridSpec(
            num_scalar_prefetch=2,
            grid=grid,
            in_specs=[
                row_block(length, width),
                whole_block((1, lanes)),
                pl.BlockSpec((width, 2 * hidden), lambda *_: (0, 0)),
                whole_block((width, width)),
            ],
            out_specs=[row_block(length, width)] + [message_block(message)] * sets,
            scratch_shapes=edge_scratch,
        ),
        out_shape=[sds(pair.shape, f32)] + [sds((message, tiles, SUB, LANES), bf16)] * sets,
        compiler_params=params(),
        cost_estimate=pl.CostEstimate(flops=edge_flops, bytes_accessed=6000000, transcendentals=0),
    )(me, token_mask, normed, live_lanes, w_tri_proj, w_tri_gate)

    left_in = [exchange(left[s], groups, s) for s in range(sets)]

    chunks = [SUB] * tiles
    total = sets * row_count
    sums = pl.pallas_call(
        functools.partial(triangle_kernel, groups, sets, per_set, full, chunks),
        name="triangle",
        grid_spec=pltpu.PrefetchScalarGridSpec(
            num_scalar_prefetch=1,
            grid=(1,),
            in_specs=[whole_block(right[0].shape)] * groups + [whole_block(left[0].shape)] * sets,
            out_specs=[whole_block((size, message, LANES)) for _ in range(sets) for size in chunks],
            scratch_shapes=[
                pltpu.VMEM((2, groups, row_count, LANES), f32),
                pltpu.VMEM((groups, row_count, LANES), f32),
                pltpu.VMEM((per_set * total, LANES), f32),
                pltpu.VMEM((per_set * total, LANES), f32),
            ],
        ),
        out_shape=[sds((size, message, LANES), bf16) for _ in range(sets) for size in chunks],
        compiler_params=params(),
        cost_estimate=pl.CostEstimate(flops=2 * per_set * total * lanes * lanes, bytes_accessed=6000000, transcendentals=0),
    )(me, *right_in, *left_in)

    attention_in = pl.pallas_call(
        functools.partial(attention_in_kernel, groups),
        name="attention_in",
        grid_spec=pltpu.PrefetchScalarGridSpec(
            num_scalar_prefetch=1,
            grid=(1,),
            in_specs=[pl.BlockSpec((slabs, tiles, SUB, LANES), lambda *_: (message // slabs, 0, 0, 0))] * groups
            + [whole_block(w_query.shape), whole_block(w_key.shape), whole_block(w_value_gate.shape)],
            out_specs=[
                whole_block((row_count, channels)),
                whole_block((length, channels)),
                whole_block((length, channels)),
                whole_block((row_count, channels)),
            ],
            scratch_shapes=[pltpu.VMEM((groups, row_count, channels), f32)],
        ),
        out_shape=[
            sds((row_count, channels), bf16),
            sds((length, channels), bf16),
            sds((length, channels), bf16),
            sds((row_count, channels), f32),
        ],
        compiler_params=params(),
        cost_estimate=pl.CostEstimate(flops=2 * length * channels * channels * 3, bytes_accessed=3000000, transcendentals=0),
    )(me, *right_in, w_query, w_key, w_value_gate)
    queries, keys, values, att_gate = attention_in

    n = len(chunks)
    outs = None
    for k in range(n):
        tri = [exchange(sums[a * n + k], groups, a) for a in range(sets)]
        at = k
        part_rows = lambda *shape: pl.BlockSpec((SUB,) + shape, lambda g, *_, at=at: (at + g,) + (0,) * len(shape))
        operands = [
            *tri, pair, gate_pair, w_tri_out.reshape(sets, per_set, width), w_trans_in, w_trans_out, w_bias,
            queries, keys, values, att_gate, live.reshape(1, length), w_out,
        ]
        in_specs = (
            [row_block(message, LANES)] * sets
            + [part_rows(length, width), part_rows(length, width), whole_block((sets, per_set, width))]
            + [whole_block(w_trans_in.shape), whole_block(w_trans_out.shape), whole_block(w_bias.shape)]
            + [part_rows(channels), whole_block(keys.shape), whole_block(values.shape), part_rows(channels)]
            + [whole_block((1, length)), whole_block(w_out.shape)]
        )
        aliases = {}
        if outs is not None:
            aliases = {1 + len(operands): 0, 2 + len(operands): 1}
            operands += list(outs)
            in_specs += [pl.BlockSpec(memory_space=pl.ANY)] * 2
        outs = pl.pallas_call(
            functools.partial(tail_kernel, sets, per_set, heads),
            name="tail",
            grid_spec=pltpu.PrefetchScalarGridSpec(
                num_scalar_prefetch=1,
                grid=(chunks[k] // SUB,),
                in_specs=in_specs,
                out_specs=[part_rows(length, width), part_rows(channels)],
                scratch_shapes=[
                    pltpu.VMEM((hidden, width), bf16),
                    pltpu.VMEM((heads, width), bf16),
                    pltpu.VMEM((SUB * heads, length), f32),
                ],
            ),
            out_shape=[sds(pair.shape, f32), sds(single.shape, f32)],
            input_output_aliases=aliases,
            compiler_params=params(),
            cost_estimate=pl.CostEstimate(
                flops=2 * SUB * length * width * (hidden + 3 * inner_width), bytes_accessed=4000000, transcendentals=0
            ),
        )(me, *operands)
    return tuple(outs)


def triangle(pieces):
    left_op, right_op = pieces
    return jnp.einsum("gcik,gcjk->gcij", left_op, right_op, preferred_element_type=jnp.float32)


def plain_body(
    pair,
    single,
    token_mask,
    w_tri_proj,
    w_tri_gate,
    w_tri_out,
    w_trans_in,
    w_trans_out,
    w_bias,
    w_query,
    w_key,
    w_value_gate,
    w_out,
):
    row_count, length, pair_width = pair.shape
    groups = lax.axis_size("row")
    hidden = w_tri_out.shape[0]
    per_dev = hidden // groups
    inner_width = w_trans_out.shape[0]
    head_count = w_bias.shape[1]
    channels = single.shape[1]
    head_size = channels // head_count
    row_start = lax.axis_index("row") * row_count
    live_all = token_mask.astype(jnp.float32)
    own_live = lax.dynamic_slice_in_dim(live_all, row_start, row_count)
    pair_live = own_live[:, None] * live_all[None, :]
    normed = layer_norm(pair, 2).astype(jnp.bfloat16)

    def operand(offset):
        weights_two = w_tri_proj[:, offset * hidden : (offset + 2) * hidden].reshape(
            pair_width, 2, groups, per_dev
        )
        projected = jnp.einsum(
            "ikd,dsgc->sgcik", normed, weights_two, preferred_element_type=jnp.float32
        )
        return (jax.nn.sigmoid(projected[1]) * projected[0] * pair_live).astype(jnp.bfloat16)

    left_edge = operand(0)
    right_edge = operand(2)
    product = triangle(
        (
            lax.all_to_all(left_edge, "row", split_axis=0, concat_axis=2, tiled=True),
            lax.all_to_all(right_edge, "row", split_axis=0, concat_axis=2, tiled=True),
        )
    )
    returned = lax.all_to_all(
        product.astype(jnp.bfloat16), "row", split_axis=2, concat_axis=0, tiled=True
    ).astype(product.dtype)
    summed = returned.reshape(hidden, row_count, length)
    triangle_normed = layer_norm(summed, 0).astype(jnp.bfloat16)
    tri_out = jnp.einsum(
        "cij,cd->ijd", triangle_normed, w_tri_out, preferred_element_type=jnp.float32
    )
    gate_pair = jax.nn.sigmoid(
        jnp.einsum("ijc,cd->ijd", normed, w_tri_gate, preferred_element_type=jnp.float32)
    )
    pair_mid = pair + gate_pair * tri_out
    block_rows = math.gcd(row_count, 8)

    def transition(row_slab):
        trans_normed = layer_norm(row_slab, 2).astype(jnp.bfloat16)
        gate_up = jnp.einsum(
            "ijc,cf->ijf", trans_normed, w_trans_in, preferred_element_type=jnp.float32
        )
        inner_act = (jax.nn.silu(gate_up[..., :inner_width]) * gate_up[..., inner_width:]).astype(
            jnp.bfloat16
        )
        return row_slab + jnp.einsum(
            "ijf,fc->ijc", inner_act, w_trans_out, preferred_element_type=jnp.float32
        )

    pair_new = lax.map(
        transition, pair_mid.reshape(row_count // block_rows, block_rows, length, pair_width)
    ).reshape(row_count, length, pair_width)
    bias_normed = layer_norm(pair_new, 2).astype(jnp.bfloat16)
    bias = jnp.einsum("ijc,ch->hij", bias_normed, w_bias, preferred_element_type=jnp.float32)
    single_normed = layer_norm(single, 1).astype(jnp.bfloat16)
    queries = jnp.dot(single_normed, w_query, preferred_element_type=jnp.float32).astype(
        jnp.bfloat16
    )
    att_gate = jax.nn.sigmoid(
        jnp.dot(single_normed, w_value_gate[:, channels:], preferred_element_type=jnp.float32)
    )
    normed_all = lax.all_gather(single_normed, "row", axis=0, tiled=True)
    keys_all = jnp.dot(normed_all, w_key, preferred_element_type=jnp.float32).astype(jnp.bfloat16)
    values_all = jnp.dot(
        normed_all, w_value_gate[:, :channels], preferred_element_type=jnp.float32
    ).astype(jnp.bfloat16)
    query_heads = queries.reshape(row_count, head_count, head_size)
    key_heads = keys_all.reshape(length, head_count, head_size)
    value_heads = values_all.reshape(length, head_count, head_size)
    scores = (
        jnp.einsum("ihd,jhd->hij", query_heads, key_heads, preferred_element_type=jnp.float32)
        / jnp.sqrt(jnp.float32(head_size))
        + bias
    )
    scores = jnp.where(live_all[None, None, :] > 0, scores, jnp.float32(-1000000000.0))
    row_max = jnp.max(scores, axis=2, keepdims=True)
    weights = jnp.exp(scores - row_max)
    weights = weights / jnp.sum(weights, axis=2, keepdims=True)
    probs = weights.astype(jnp.bfloat16)
    attended = jnp.einsum(
        "hij,jhd->ihd", probs, value_heads, preferred_element_type=jnp.float32
    ).reshape(row_count, channels)
    gated = (att_gate * attended).astype(jnp.bfloat16)
    single_update = jnp.dot(gated, w_out, preferred_element_type=jnp.float32)
    return (pair_new, single_update)


def body(*arrays):
    pair, single, w_tri_out = arrays[0], arrays[1], arrays[5]
    row_count, length, _ = pair.shape
    groups = lax.axis_size("row")
    hidden = w_tri_out.shape[0]
    sets = groups // 2
    packs = (
        groups >= 4
        and groups & (groups - 1) == 0
        and hidden % (32 * sets) == 0
        and (length % LANES) * 2 == LANES
        and length // LANES == 1
        and row_count % SUB == 0
        and single.shape[1] % LANES == 0
        and (hidden // sets * 3 // 2) % (single.shape[1] // LANES) == 0
    )
    return (fast_body if packs else plain_body)(*arrays)


def solution(mesh):
    in_specs = (
        P(("crop", "row"), None, None),
        P(("crop", "row"), None),
        P("crop"),
        P(),
        P(),
        P(),
        P(),
        P(),
        P(),
        P(),
        P(),
        P(),
        P(),
    )
    out_specs = (P(("crop", "row"), None, None), P(("crop", "row"), None))
    return jax.shard_map(body, mesh=mesh, in_specs=in_specs, out_specs=out_specs, check_vma=False)
```

```python
import functools
import math

import jax
import jax.numpy as jnp
from jax import lax
from jax.experimental import pallas as pl
from jax.experimental.pallas import tpu as pltpu
from jax.sharding import PartitionSpec as P


epsilon = 1e-05
LANES = 128
SUB = 8
f32 = jnp.float32
bf16 = jnp.bfloat16
NT = (((1,), (1,)), ((), ()))


def layer_norm(values_in, along):
    average = jnp.mean(values_in, axis=along, keepdims=True)
    centered = values_in - average
    spread = jnp.mean(centered * centered, axis=along, keepdims=True)
    return centered * lax.rsqrt(spread + epsilon)


def sigmoid(x):
    return 0.5 * jnp.tanh(0.5 * x) + 0.5


def repeat_rest(x, full):
    return jnp.concatenate([x, x[full:]], axis=0)


def first_half_lanes(shape):
    return lax.broadcasted_iota(jnp.int32, shape, len(shape) - 1) < LANES // 2


def edges_to_messages(me_ref, mask_ref, live_ref, wt_ref, rows_of, head_ref, rest_ref, out_refs, first, hidden, full):
    sets = len(out_refs)
    per_set = hidden // sets
    pairs = per_set // 2
    stride = hidden + SUB
    own_set = lax.rem(me_ref[0], sets)
    tokens = live_ref[...].astype(f32).reshape(1, live_ref.shape[0])
    tokens = jnp.concatenate([tokens, tokens[:, full:]], axis=1)
    for j in range(SUB):
        x = repeat_rest(rows_of(j), full)
        projected = lax.dot_general(wt_ref[...], x, NT, preferred_element_type=f32)
        live = tokens * mask_ref[first + j].astype(f32)
        edge = sigmoid(projected[hidden:]) * projected[:hidden] * live
        for s in range(sets):
            q = lax.bitwise_xor(own_set, s)
            at = pl.multiple_of(j * stride + q * per_set, SUB)
            part = edge[s * per_set : (s + 1) * per_set]
            head_ref[pl.ds(at, per_set), :] = part[:, :LANES]
            rest_ref[pl.ds(at, per_set), :] = part[:, LANES:]
    low = first_half_lanes((SUB, LANES))
    for q in range(sets):
        for c in range(pairs):
            a = pl.ds(q * per_set + c, SUB, stride=stride)
            b = pl.ds(q * per_set + pairs + c, SUB, stride=stride)
            out_refs[q][c, 0] = head_ref[a, :].astype(bf16)
            out_refs[q][pairs + c, 0] = head_ref[b, :].astype(bf16)
            out_refs[q][per_set + c, 0] = jnp.where(low, rest_ref[a, :], rest_ref[b, :]).astype(bf16)


def right_kernel(hidden, full, sets, row_count, offset, me_ref, mask_ref, pair_ref, single_ref, live_ref, w_ref, *rest):
    out_refs = rest[-3 - sets : -3]
    head_ref, rest_ref, wt_ref = rest[-3:]

    @pl.when(pl.program_id(0) == 0)
    def _():
        wt_ref[...] = w_ref[...].T

    first = me_ref[0] * row_count + offset + pl.program_id(0) * SUB
    rows_of = lambda j: layer_norm(pair_ref[j], 1).astype(bf16)
    edges_to_messages(me_ref, mask_ref, live_ref, wt_ref, rows_of, head_ref, rest_ref, out_refs, first, hidden, full)
    single_normed = layer_norm(single_ref[...], 1).astype(bf16)
    slabs = single_ref.shape[1] // LANES
    base = hidden // sets * 3 // 2
    for q in range(sets):
        for t in range(slabs):
            out_refs[q][base + t, 0] = single_normed[:, t * LANES : (t + 1) * LANES]


def left_kernel(hidden, full, sets, row_count, me_ref, mask_ref, pair_ref, live_ref, w_ref, *rest):
    out_refs = rest[-3 - sets : -3]
    head_ref, rest_ref, wt_ref = rest[-3:]

    @pl.when(pl.program_id(0) == 0)
    def _():
        wt_ref[...] = w_ref[...].T

    first = me_ref[0] * row_count + pl.program_id(0) * SUB
    rows_of = lambda j: layer_norm(pair_ref[j], 1).astype(bf16)
    edges_to_messages(me_ref, mask_ref, live_ref, wt_ref, rows_of, head_ref, rest_ref, out_refs, first, hidden, full)


def gate_kernel(pair_ref, w_gate_ref, _, gate_ref):
    rows = pair_ref.shape[0] * pair_ref.shape[1]
    x = layer_norm(pair_ref[...].reshape(rows, pair_ref.shape[2]), 1).astype(bf16)
    gate_ref[...] = sigmoid(jnp.dot(x, w_gate_ref[...], preferred_element_type=f32)).reshape(gate_ref.shape)


def plain_rows(block):
    wide = block.astype(f32)
    return wide.reshape(wide.shape[0] * wide.shape[1], wide.shape[2])


def triangle_kernel(groups, sets, per_set, me_ref, *refs):
    right_refs, left_refs = refs[:groups], refs[groups : groups + sets]
    out_refs = refs[-sets - 3 : -3]
    head_ref, rest_ref, sums_ref = refs[-3:]
    pairs = per_set // 2
    rows = left_refs[0].shape[1] * SUB
    here = right_refs[0].shape[1] * SUB
    columns = groups * here
    me = me_ref[0]
    total = sets * rows
    stride = total + SUB
    low = first_half_lanes((total, LANES))
    fill = lambda x: x if columns == LANES else jnp.concatenate([x, x], axis=0)
    for s in range(groups):
        d = lax.bitwise_xor(me, s)
        wide = right_refs[s][: per_set + pairs].astype(f32).reshape(per_set + pairs, here, LANES)
        head_ref[:, d] = wide[:per_set]
        rest_ref[:, d] = wide[per_set:]
    for c in range(pairs):
        right_rest = fill(rest_ref[c].reshape(columns, LANES)).astype(bf16)
        left_rest = jnp.concatenate([plain_rows(r[per_set + c]) for r in left_refs], axis=0)
        for p in range(2):
            channel = p * pairs + c
            right = fill(head_ref[channel].reshape(columns, LANES)).astype(bf16)
            left = jnp.concatenate([plain_rows(r[channel]) for r in left_refs], axis=0).astype(bf16)
            kept = jnp.where(low if p == 0 else jnp.logical_not(low), left_rest, 0.0).astype(bf16)
            sums_ref[channel * stride : channel * stride + total, :] = lax.dot_general(
                jnp.concatenate([left, kept], axis=1),
                jnp.concatenate([right, right_rest], axis=1),
                NT,
                preferred_element_type=f32,
            )
    low_half = first_half_lanes((pairs, LANES))
    for a in range(sets):
        for i in range(rows):
            x = sums_ref[pl.ds(a * rows + i, per_set, stride=stride), :]
            if columns < LANES:
                x = jnp.where(low_half, x[:pairs], x[pairs:])
            out_refs[a][i] = x.astype(bf16)


def attention_in_kernel(groups, chunks, me_ref, *refs):
    n = len(chunks)
    right_refs = refs[: groups * n]
    w_query_ref, w_key_ref, w_value_gate_ref, q_ref, g_ref = refs[groups * n : groups * n + 5]
    k_refs = refs[groups * n + 5 : groups * n + 5 + n]
    v_refs = refs[groups * n + 5 + n : groups * n + 5 + 2 * n]
    all_refs = refs[groups * n + 5 + 2 * n :]
    channels = w_query_ref.shape[0]
    me = me_ref[0]
    for k in range(n):
        for s in range(groups):
            d = lax.bitwise_xor(me, s)
            for t in range(channels // LANES):
                all_refs[k][d, :, t * LANES : (t + 1) * LANES] = plain_rows(right_refs[k * groups + s][t])
    own = jnp.concatenate([r[me] for r in all_refs], axis=0).astype(bf16)
    q_ref[...] = jnp.dot(own, w_query_ref[...], preferred_element_type=f32).astype(bf16)
    g_ref[...] = sigmoid(jnp.dot(own, w_value_gate_ref[:, channels:], preferred_element_type=f32))
    for k in range(n):
        every = all_refs[k][...].reshape(k_refs[k].shape).astype(bf16)
        k_refs[k][...] = jnp.dot(every, w_key_ref[...], preferred_element_type=f32).astype(bf16)
        v_refs[k][...] = jnp.dot(every, w_value_gate_ref[:, :channels], preferred_element_type=f32).astype(bf16)


def tail_kernel(sets, per_set, heads, slab, attends, me_ref, *refs):
    tri_refs = refs[:sets]
    pair_ref, gate_ref, w_tri_out_ref, w_in_ref, w_down_ref, w_bias_ref = refs[sets : sets + 6]
    if attends:
        new_ref, single_ref, bias_ref, w_rel_ref, wb_ref = refs[-5:]
    else:
        new_ref, bias_ref, w_rel_ref, wb_ref = refs[-4:]
    width = pair_ref.shape[-1]
    columns = math.prod(pair_ref.shape[1:-1])
    together = LANES // columns
    inner_width = w_down_ref.shape[0]
    me = me_ref[0]

    @pl.when(pl.program_id(0) == 0)
    def _():
        own_set = lax.rem(me, sets)
        for a in range(sets):
            w_rel_ref[a * per_set : (a + 1) * per_set] = w_tri_out_ref[lax.bitwise_xor(own_set, a)]
        wb_ref[...] = w_bias_ref[...].T

    low = first_half_lanes((per_set // 2, LANES))

    def sums_of(i):
        parts = []
        for r in tri_refs:
            if together == 1:
                parts.append(r[i].astype(f32))
            else:
                here, there = r[i].astype(f32), r[i + 1].astype(f32)
                parts.append(jnp.where(low, here, pltpu.roll(there, LANES // 2, 1)))
                parts.append(jnp.where(low, pltpu.roll(here, LANES // 2, 1), there))
        return jnp.concatenate(parts, axis=0)

    def rows(b, carry):
        i = b * slab * together
        tri = []
        for n in range(slab):
            tri.append(layer_norm(sums_of(i + n * together), 0).astype(bf16).T)
        tri = jnp.concatenate(tri, axis=0)
        tri_out = jnp.dot(tri, w_rel_ref[...], preferred_element_type=f32)
        here = pl.ds(i, slab * together)
        block = (slab * LANES, width)
        mid = pair_ref[here].reshape(block) + gate_ref[here].reshape(block) * tri_out
        trans = layer_norm(mid, 1).astype(bf16)
        gate_up = jnp.dot(trans, w_in_ref[...], preferred_element_type=f32)
        gate = gate_up[:, :inner_width]
        inner = (gate * sigmoid(gate) * gate_up[:, inner_width:]).astype(bf16)
        new = mid + jnp.dot(inner, w_down_ref[...], preferred_element_type=f32)
        new_ref[here] = new.reshape((slab * together,) + new_ref.shape[1:])
        normed = layer_norm(new, 1).astype(bf16)
        bias = lax.dot_general(wb_ref[...], normed, NT, preferred_element_type=f32)
        for n in range(slab):
            part = bias[:, n * LANES : (n + 1) * LANES]
            bias_ref[i + n * together] = part
            if together == 2:
                bias_ref[i + n * together + 1] = pltpu.roll(part, LANES // 2, 1)
        return carry

    lax.fori_loop(0, pair_ref.shape[0] // (slab * together), rows, 0)
    if attends:
        attention(heads, attends, refs[sets + 6 :], bias_ref, single_ref)


def attention(heads, n, refs, last_bias_ref, single_ref):
    q_ref, g_ref, w_out_ref = refs[:3]
    k_refs, v_refs, live_refs = refs[3 : 3 + n], refs[3 + n : 3 + 2 * n], refs[3 + 2 * n : 3 + 3 * n]
    bias_refs = [*refs[3 + 3 * n : 2 + 4 * n], last_bias_ref]
    row_count, channels = q_ref.shape
    head_size = channels // heads
    of_head = lax.broadcasted_iota(jnp.int32, (row_count, heads, channels), 1)
    lane = lax.broadcasted_iota(jnp.int32, (row_count, heads, channels), 2)
    mine = jnp.logical_and(lane >= of_head * head_size, lane < (of_head + 1) * head_size)
    spread = jnp.where(mine, jnp.broadcast_to(q_ref[...].astype(f32)[:, None, :], mine.shape), 0.0)
    spread = spread.reshape(row_count * heads, channels).astype(bf16)
    scores = []
    for k in range(n):
        part = lax.dot_general(spread, k_refs[k][...], NT, preferred_element_type=f32)
        bias = bias_refs[k][...].reshape(row_count * heads, LANES)[:, : part.shape[1]]
        part = part / jnp.sqrt(f32(head_size)) + bias
        scores.append(jnp.where(live_refs[k][...] > 0, part, f32(-1000000000.0)))
    row_max = functools.reduce(jnp.maximum, [jnp.max(x, axis=1, keepdims=True) for x in scores])
    weights = [jnp.exp(x - row_max) for x in scores]
    row_sum = sum(jnp.sum(x, axis=1, keepdims=True) for x in weights)
    attended = sum(
        jnp.dot((x / row_sum).astype(bf16), v[...], preferred_element_type=f32) for x, v in zip(weights, v_refs)
    )
    attended = jnp.sum(jnp.where(mine, attended.reshape(mine.shape), 0.0), axis=1)
    gated = (g_ref[...] * attended).astype(bf16)
    single_ref[...] = jnp.dot(gated, w_out_ref[...], preferred_element_type=f32)


def whole_block(shape):
    return pl.BlockSpec(shape, lambda *_: (0,) * len(shape))


def params():
    return pltpu.CompilerParams(dimension_semantics=("arbitrary",))


def anywhere(arrays):
    return [pl.BlockSpec(memory_space=pl.ANY)] * len(arrays)


def cost(flops):
    return pl.CostEstimate(flops=int(flops), bytes_accessed=4000000, transcendentals=0)


def exchange(x, groups, s):
    return x if s == 0 else lax.ppermute(x, "row", [(r, r ^ s) for r in range(groups)])


def chunk_tiles(tiles, groups):
    most = LANES // (groups * SUB)
    chunks = [most] * (tiles // most) if most else []
    return chunks + ([tiles % most] if most and tiles % most else [])


def fast_body(
    pair, single, token_mask, w_tri_proj, w_tri_gate, w_tri_out, w_trans_in, w_trans_out, w_bias, w_query, w_key, w_value_gate, w_out
):
    row_count, length, width = pair.shape
    groups = lax.axis_size("row")
    sets = groups // 2
    hidden = w_tri_out.shape[0]
    per_set = hidden // sets
    message = per_set * 3 // 2
    inner_width = w_trans_out.shape[0]
    heads = w_bias.shape[1]
    channels = single.shape[1]
    slabs = channels // LANES
    full = length // LANES * LANES
    lanes = full + LANES
    tiles = row_count // SUB
    chunks = chunk_tiles(tiles, groups)
    starts = [sum(chunks[:k]) for k in range(len(chunks))]
    me = lax.axis_index("row").astype(jnp.int32).reshape(1)
    live = token_mask.astype(f32)
    sds = jax.ShapeDtypeStruct
    message_block = lambda n: pl.BlockSpec((n, 1, SUB, LANES), lambda g, *_: (0, g, 0, 0))
    edge_scratch = [pltpu.VMEM((SUB * (hidden + SUB), LANES), f32)] * 2 + [pltpu.VMEM((2 * hidden, width), bf16)]
    edge_flops = 2 * SUB * lanes * width * 2 * hidden

    def right_edges(k, after):
        at = starts[k]
        return pl.pallas_call(
            functools.partial(right_kernel, hidden, full, sets, row_count, at * SUB),
            name="right",
            grid_spec=pltpu.PrefetchScalarGridSpec(
                num_scalar_prefetch=2,
                grid=(chunks[k],),
                in_specs=[
                    pl.BlockSpec((SUB, length, width), lambda g, *_: (at + g, 0, 0)),
                    pl.BlockSpec((SUB, channels), lambda g, *_: (at + g, 0)),
                    whole_block((length,)),
                    pl.BlockSpec((width, 2 * hidden), lambda *_: (0, 1)),
                ]
                + anywhere(after),
                out_specs=[message_block(message + slabs)] * sets,
                scratch_shapes=edge_scratch,
            ),
            out_shape=[sds((message + slabs, chunks[k], SUB, LANES), bf16)] * sets,
            compiler_params=params(),
            cost_estimate=cost(edge_flops * chunks[k]),
        )(me, token_mask, pair, single, token_mask, w_tri_proj, *after)

    def left_edges(after):
        return pl.pallas_call(
            functools.partial(left_kernel, hidden, full, sets, row_count),
            name="left",
            grid_spec=pltpu.PrefetchScalarGridSpec(
                num_scalar_prefetch=2,
                grid=(tiles,),
                in_specs=[
                    pl.BlockSpec((SUB, length, width), lambda g, *_: (g, 0, 0)),
                    whole_block((length,)),
                    pl.BlockSpec((width, 2 * hidden), lambda *_: (0, 0)),
                ]
                + anywhere(after),
                out_specs=[message_block(message)] * sets,
                scratch_shapes=edge_scratch,
            ),
            out_shape=[sds((message, tiles, SUB, LANES), bf16)] * sets,
            compiler_params=params(),
            cost_estimate=cost(edge_flops * tiles),
        )(me, token_mask, pair, token_mask, w_tri_proj, *after)

    right_in, left_in, after = [], None, []
    for k in range(len(chunks)):
        right = right_edges(k, after)
        right_in.append([exchange(right[s % sets], groups, s) for s in range(groups)])
        after = [right[0]]
        if left_in is None:
            left = left_edges(after)
            left_in = [exchange(left[s], groups, s) for s in range(sets)]
            after = [left[0]]

    gate_pair = pl.pallas_call(
        gate_kernel,
        name="gate",
        grid=(tiles,),
        in_specs=[pl.BlockSpec((SUB, length, width), lambda g: (g, 0, 0)), whole_block((width, width))] + anywhere(after),
        out_specs=pl.BlockSpec((SUB, length, width), lambda g: (g, 0, 0)),
        out_shape=sds(pair.shape, f32),
        compiler_params=params(),
        cost_estimate=cost(2 * row_count * length * width * width),
    )(pair, w_tri_gate, *after)

    total = sets * row_count
    tri_in = []
    for k in range(len(chunks)):
        columns = groups * chunks[k] * SUB
        sums_shape = (row_count, per_set * columns // LANES, LANES)
        sums = pl.pallas_call(
            functools.partial(triangle_kernel, groups, sets, per_set),
            name="triangle",
            grid_spec=pltpu.PrefetchScalarGridSpec(
                num_scalar_prefetch=1,
                grid=(1,),
                in_specs=[whole_block((message, chunks[k], SUB, LANES))] * groups
                + [whole_block((message, tiles, SUB, LANES))] * sets
                + anywhere([gate_pair]),
                out_specs=[whole_block(sums_shape)] * sets,
                scratch_shapes=[
                    pltpu.VMEM((per_set, groups, chunks[k] * SUB, LANES), f32),
                    pltpu.VMEM((per_set // 2, groups, chunks[k] * SUB, LANES), f32),
                    pltpu.VMEM((per_set * (total + SUB), LANES), f32),
                ],
            ),
            out_shape=[sds(sums_shape, bf16)] * sets,
            compiler_params=params(),
            cost_estimate=cost(2 * per_set * total * lanes * LANES),
        )(me, *right_in[k], *left_in, gate_pair)
        tri_in.append([exchange(sums[a], groups, a) for a in range(sets)])

    tokens = [groups * n * SUB for n in chunks]
    queries, att_gate, *keys_values = pl.pallas_call(
        functools.partial(attention_in_kernel, groups, chunks),
        name="attention_in",
        grid_spec=pltpu.PrefetchScalarGridSpec(
            num_scalar_prefetch=1,
            grid=(1,),
            in_specs=[
                pl.BlockSpec((slabs, n, SUB, LANES), lambda *_: (message // slabs, 0, 0, 0))
                for n in chunks
                for _ in range(groups)
            ]
            + [whole_block(w_query.shape), whole_block(w_key.shape), whole_block(w_value_gate.shape)],
            out_specs=[whole_block((row_count, channels))] * 2 + [whole_block((n, channels)) for n in tokens + tokens],
            scratch_shapes=[pltpu.VMEM((groups, n * SUB, channels), f32) for n in chunks],
        ),
        out_shape=[sds((row_count, channels), bf16), sds((row_count, channels), f32)]
        + [sds((n, channels), bf16) for n in tokens + tokens],
        compiler_params=params(),
        cost_estimate=cost(2 * length * channels * channels * 3),
    )(me, *[x for part in right_in for x in part], w_query, w_key, w_value_gate)

    tiled = (row_count, groups, tiles, SUB, width)
    pair_tiled, gate_tiled = pair.reshape(tiled), gate_pair.reshape(tiled)
    new, biases = None, []
    lives = [
        live.reshape(groups, tiles, SUB)[:, at : at + n].reshape(1, groups * n * SUB) for at, n in zip(starts, chunks)
    ]
    for k, n in enumerate(chunks):
        attends = len(chunks) if k == len(chunks) - 1 else 0
        columns = tokens[k]
        together = LANES // columns
        take = row_count if attends else SUB
        slab = take // together
        at = starts[k] // n
        part_rows = pl.BlockSpec((take, groups, n, SUB, width), lambda g, *_, at=at: (g, 0, at, 0, 0))
        operands = [*tri_in[k], pair_tiled, gate_tiled, w_tri_out.reshape(sets, per_set, width), w_trans_in, w_trans_out, w_bias]
        sums_block = (take,) + tri_in[k][0].shape[1:]
        in_specs = [pl.BlockSpec(sums_block, lambda g, *_: (g, 0, 0))] * sets + [part_rows, part_rows]
        if attends:
            operands += [queries, att_gate, w_out, *keys_values, *lives, *biases]
        in_specs += [whole_block(x.shape) for x in operands[sets + 2 :]]
        aliases = {}
        if new is not None:
            aliases = {1 + len(operands): 0}
            operands.append(new)
            in_specs += anywhere([new])
        bias_shape = (row_count, heads, LANES)
        weights = [pltpu.VMEM((hidden, width), bf16), pltpu.VMEM((heads, width), bf16)]
        new, last = pl.pallas_call(
            functools.partial(tail_kernel, sets, per_set, heads, slab, attends),
            name="tail",
            grid_spec=pltpu.PrefetchScalarGridSpec(
                num_scalar_prefetch=1,
                grid=(row_count // take,),
                in_specs=in_specs,
                out_specs=[
                    part_rows,
                    whole_block(single.shape) if attends else pl.BlockSpec((SUB, heads, LANES), lambda g, *_: (g, 0, 0)),
                ],
                scratch_shapes=([pltpu.VMEM(bias_shape, f32)] if attends else []) + weights,
            ),
            out_shape=[sds(tiled, f32), sds(single.shape if attends else bias_shape, f32)],
            input_output_aliases=aliases,
            compiler_params=params(),
            cost_estimate=cost(2 * row_count * columns * width * (hidden + 3 * inner_width)),
        )(me, *operands)
        biases.append(last)
    return new.reshape(pair.shape), last


def triangle(pieces):
    left_op, right_op = pieces
    return jnp.einsum("gcik,gcjk->gcij", left_op, right_op, preferred_element_type=jnp.float32)


def plain_body(
    pair,
    single,
    token_mask,
    w_tri_proj,
    w_tri_gate,
    w_tri_out,
    w_trans_in,
    w_trans_out,
    w_bias,
    w_query,
    w_key,
    w_value_gate,
    w_out,
):
    row_count, length, pair_width = pair.shape
    groups = lax.axis_size("row")
    hidden = w_tri_out.shape[0]
    per_dev = hidden // groups
    inner_width = w_trans_out.shape[0]
    head_count = w_bias.shape[1]
    channels = single.shape[1]
    head_size = channels // head_count
    row_start = lax.axis_index("row") * row_count
    live_all = token_mask.astype(jnp.float32)
    own_live = lax.dynamic_slice_in_dim(live_all, row_start, row_count)
    pair_live = own_live[:, None] * live_all[None, :]
    normed = layer_norm(pair, 2).astype(jnp.bfloat16)

    def operand(offset):
        weights_two = w_tri_proj[:, offset * hidden : (offset + 2) * hidden].reshape(
            pair_width, 2, groups, per_dev
        )
        projected = jnp.einsum(
            "ikd,dsgc->sgcik", normed, weights_two, preferred_element_type=jnp.float32
        )
        return (jax.nn.sigmoid(projected[1]) * projected[0] * pair_live).astype(jnp.bfloat16)

    left_edge = operand(0)
    right_edge = operand(2)
    product = triangle(
        (
            lax.all_to_all(left_edge, "row", split_axis=0, concat_axis=2, tiled=True),
            lax.all_to_all(right_edge, "row", split_axis=0, concat_axis=2, tiled=True),
        )
    )
    returned = lax.all_to_all(
        product.astype(jnp.bfloat16), "row", split_axis=2, concat_axis=0, tiled=True
    ).astype(product.dtype)
    summed = returned.reshape(hidden, row_count, length)
    triangle_normed = layer_norm(summed, 0).astype(jnp.bfloat16)
    tri_out = jnp.einsum(
        "cij,cd->ijd", triangle_normed, w_tri_out, preferred_element_type=jnp.float32
    )
    gate_pair = jax.nn.sigmoid(
        jnp.einsum("ijc,cd->ijd", normed, w_tri_gate, preferred_element_type=jnp.float32)
    )
    pair_mid = pair + gate_pair * tri_out
    block_rows = math.gcd(row_count, 8)

    def transition(row_slab):
        trans_normed = layer_norm(row_slab, 2).astype(jnp.bfloat16)
        gate_up = jnp.einsum(
            "ijc,cf->ijf", trans_normed, w_trans_in, preferred_element_type=jnp.float32
        )
        inner_act = (jax.nn.silu(gate_up[..., :inner_width]) * gate_up[..., inner_width:]).astype(
            jnp.bfloat16
        )
        return row_slab + jnp.einsum(
            "ijf,fc->ijc", inner_act, w_trans_out, preferred_element_type=jnp.float32
        )

    pair_new = lax.map(
        transition, pair_mid.reshape(row_count // block_rows, block_rows, length, pair_width)
    ).reshape(row_count, length, pair_width)
    bias_normed = layer_norm(pair_new, 2).astype(jnp.bfloat16)
    bias = jnp.einsum("ijc,ch->hij", bias_normed, w_bias, preferred_element_type=jnp.float32)
    single_normed = layer_norm(single, 1).astype(jnp.bfloat16)
    queries = jnp.dot(single_normed, w_query, preferred_element_type=jnp.float32).astype(
        jnp.bfloat16
    )
    att_gate = jax.nn.sigmoid(
        jnp.dot(single_normed, w_value_gate[:, channels:], preferred_element_type=jnp.float32)
    )
    normed_all = lax.all_gather(single_normed, "row", axis=0, tiled=True)
    keys_all = jnp.dot(normed_all, w_key, preferred_element_type=jnp.float32).astype(jnp.bfloat16)
    values_all = jnp.dot(
        normed_all, w_value_gate[:, :channels], preferred_element_type=jnp.float32
    ).astype(jnp.bfloat16)
    query_heads = queries.reshape(row_count, head_count, head_size)
    key_heads = keys_all.reshape(length, head_count, head_size)
    value_heads = values_all.reshape(length, head_count, head_size)
    scores = (
        jnp.einsum("ihd,jhd->hij", query_heads, key_heads, preferred_element_type=jnp.float32)
        / jnp.sqrt(jnp.float32(head_size))
        + bias
    )
    scores = jnp.where(live_all[None, None, :] > 0, scores, jnp.float32(-1000000000.0))
    row_max = jnp.max(scores, axis=2, keepdims=True)
    weights = jnp.exp(scores - row_max)
    weights = weights / jnp.sum(weights, axis=2, keepdims=True)
    probs = weights.astype(jnp.bfloat16)
    attended = jnp.einsum(
        "hij,jhd->ihd", probs, value_heads, preferred_element_type=jnp.float32
    ).reshape(row_count, channels)
    gated = (att_gate * attended).astype(jnp.bfloat16)
    single_update = jnp.dot(gated, w_out, preferred_element_type=jnp.float32)
    return (pair_new, single_update)


def body(*arrays):
    pair, single, w_tri_out = arrays[0], arrays[1], arrays[5]
    row_count, length, _ = pair.shape
    groups = lax.axis_size("row")
    hidden = w_tri_out.shape[0]
    sets = groups // 2
    packs = (
        groups >= 4
        and groups & (groups - 1) == 0
        and hidden % (32 * sets) == 0
        and (length % LANES) * 2 == LANES
        and length // LANES == 1
        and row_count % SUB == 0
        and single.shape[1] % LANES == 0
        and (hidden // sets * 3 // 2) % (single.shape[1] // LANES) == 0
        and all(groups * n * SUB in (LANES, LANES // 2) for n in chunk_tiles(row_count // SUB, groups))
        and bool(chunk_tiles(row_count // SUB, groups))
    )
    if not packs:
        return plain_body(*arrays)
    return fast_body(*arrays)


def solution(mesh):
    in_specs = (
        P(("crop", "row"), None, None),
        P(("crop", "row"), None),
        P("crop"),
        P(),
        P(),
        P(),
        P(),
        P(),
        P(),
        P(),
        P(),
        P(),
        P(),
    )
    out_specs = (P(("crop", "row"), None, None), P(("crop", "row"), None))
    return jax.shard_map(body, mesh=mesh, in_specs=in_specs, out_specs=out_specs, check_vma=False)
```

```python
import functools
import math

import jax
import jax.numpy as jnp
from jax import lax
from jax.experimental import pallas as pl
from jax.experimental.pallas import tpu as pltpu
from jax.sharding import PartitionSpec as P


epsilon = 1e-05
LANES = 128
SUB = 8
f32 = jnp.float32
bf16 = jnp.bfloat16
NT = (((1,), (1,)), ((), ()))


def layer_norm(values_in, along):
    average = jnp.mean(values_in, axis=along, keepdims=True)
    centered = values_in - average
    spread = jnp.mean(centered * centered, axis=along, keepdims=True)
    return centered * lax.rsqrt(spread + epsilon)


def sigmoid(x):
    return 0.5 * jnp.tanh(0.5 * x) + 0.5


def repeat_rest(x, full):
    return jnp.concatenate([x, x[full:]], axis=0)


def first_half_lanes(shape):
    return lax.broadcasted_iota(jnp.int32, shape, len(shape) - 1) < LANES // 2


def edges_to_messages(me_ref, mask_ref, live_ref, wt_ref, rows_of, head_ref, rest_ref, out_refs, first, hidden, full):
    sets = len(out_refs)
    per_set = hidden // sets
    pairs = per_set // 2
    stride = hidden + SUB
    own_set = lax.rem(me_ref[0], sets)
    tokens = live_ref[...].astype(f32).reshape(1, live_ref.shape[0])
    tokens = jnp.concatenate([tokens, tokens[:, full:]], axis=1)
    for j in range(SUB):
        x = repeat_rest(rows_of(j), full)
        projected = lax.dot_general(wt_ref[...], x, NT, preferred_element_type=f32)
        live = tokens * mask_ref[first + j].astype(f32)
        edge = sigmoid(projected[hidden:]) * projected[:hidden] * live
        for s in range(sets):
            q = lax.bitwise_xor(own_set, s)
            at = pl.multiple_of(j * stride + q * per_set, SUB)
            part = edge[s * per_set : (s + 1) * per_set]
            head_ref[pl.ds(at, per_set), :] = part[:, :LANES]
            rest_ref[pl.ds(at, per_set), :] = part[:, LANES:]
    low = first_half_lanes((SUB, LANES))
    for q in range(sets):
        for c in range(pairs):
            a = pl.ds(q * per_set + c, SUB, stride=stride)
            b = pl.ds(q * per_set + pairs + c, SUB, stride=stride)
            out_refs[q][c, 0] = head_ref[a, :].astype(bf16)
            out_refs[q][pairs + c, 0] = head_ref[b, :].astype(bf16)
            out_refs[q][per_set + c, 0] = jnp.where(low, rest_ref[a, :], rest_ref[b, :]).astype(bf16)


def single_places(shape, tiles):
    pieces = shape[1] // LANES * (shape[0] // SUB)
    return {n: divmod(n, tiles) for n in range(pieces)}


def single_slabs(shape, tiles, message):
    least = -(-(shape[1] // LANES * (shape[0] // SUB)) // tiles)
    return next(n for n in range(least, message + 1) if message % n == 0)


def right_kernel(hidden, full, sets, row_count, offset, single_tiles, me_ref, mask_ref, pair_ref, single_ref, live_ref, w_ref, *rest):
    out_refs = rest[-3 - sets : -3]
    head_ref, rest_ref, wt_ref = rest[-3:]

    @pl.when(pl.program_id(0) == 0)
    def _():
        wt_ref[...] = w_ref[...].T

    first = me_ref[0] * row_count + offset + pl.program_id(0) * SUB
    rows_of = lambda j: layer_norm(pair_ref[j], 1).astype(bf16)
    edges_to_messages(me_ref, mask_ref, live_ref, wt_ref, rows_of, head_ref, rest_ref, out_refs, first, hidden, full)
    if single_tiles:
        single_normed = layer_norm(single_ref[...], 1)
        base = hidden // sets * 3 // 2
        for g in range(single_tiles):

            @pl.when(pl.program_id(0) == g)
            def _():
                for n, (slab, tile) in single_places(single_ref.shape, single_tiles).items():
                    if tile == g:
                        t, at = divmod(n, row_count // SUB)
                        part = single_normed[at * SUB : (at + 1) * SUB, t * LANES : (t + 1) * LANES].astype(bf16)
                        for q in range(sets):
                            out_refs[q][base + slab, 0] = part


def left_kernel(hidden, full, sets, row_count, me_ref, mask_ref, pair_ref, live_ref, w_ref, *rest):
    out_refs = rest[-3 - sets : -3]
    head_ref, rest_ref, wt_ref = rest[-3:]

    @pl.when(pl.program_id(0) == 0)
    def _():
        wt_ref[...] = w_ref[...].T

    first = me_ref[0] * row_count + pl.program_id(0) * SUB
    rows_of = lambda j: layer_norm(pair_ref[j], 1).astype(bf16)
    edges_to_messages(me_ref, mask_ref, live_ref, wt_ref, rows_of, head_ref, rest_ref, out_refs, first, hidden, full)


def gate_kernel(pair_ref, w_gate_ref, _, gate_ref):
    rows = pair_ref.shape[0] * pair_ref.shape[1]
    x = layer_norm(pair_ref[...].reshape(rows, pair_ref.shape[2]), 1).astype(bf16)
    gate_ref[...] = sigmoid(jnp.dot(x, w_gate_ref[...], preferred_element_type=f32)).reshape(gate_ref.shape)


def plain_rows(block):
    wide = block.astype(f32)
    return wide.reshape(wide.shape[0] * wide.shape[1], wide.shape[2])


def triangle_kernel(groups, sets, per_set, me_ref, *refs):
    right_refs, left_refs = refs[:groups], refs[groups : groups + sets]
    out_refs = refs[-sets - 3 : -3]
    head_ref, rest_ref, sums_ref = refs[-3:]
    pairs = per_set // 2
    rows = left_refs[0].shape[1] * SUB
    here = right_refs[0].shape[1] * SUB
    columns = groups * here
    me = me_ref[0]
    total = sets * rows
    stride = total + SUB
    low = first_half_lanes((total, LANES))
    fill = lambda x: x if columns == LANES else jnp.concatenate([x, x], axis=0)
    for s in range(groups):
        d = lax.bitwise_xor(me, s)
        wide = right_refs[s][: per_set + pairs].astype(f32).reshape(per_set + pairs, here, LANES)
        head_ref[:, d] = wide[:per_set]
        rest_ref[:, d] = wide[per_set:]
    for c in range(pairs):
        right_rest = fill(rest_ref[c].reshape(columns, LANES)).astype(bf16)
        left_rest = jnp.concatenate([plain_rows(r[per_set + c]) for r in left_refs], axis=0)
        for p in range(2):
            channel = p * pairs + c
            right = fill(head_ref[channel].reshape(columns, LANES)).astype(bf16)
            left = jnp.concatenate([plain_rows(r[channel]) for r in left_refs], axis=0).astype(bf16)
            kept = jnp.where(low if p == 0 else jnp.logical_not(low), left_rest, 0.0).astype(bf16)
            sums_ref[channel * stride : channel * stride + total, :] = lax.dot_general(
                jnp.concatenate([left, kept], axis=1),
                jnp.concatenate([right, right_rest], axis=1),
                NT,
                preferred_element_type=f32,
            )
    low_half = first_half_lanes((pairs, LANES))
    for a in range(sets):
        for i in range(rows):
            x = sums_ref[pl.ds(a * rows + i, per_set, stride=stride), :]
            if columns < LANES:
                x = jnp.where(low_half, x[:pairs], x[pairs:])
            out_refs[a][i] = x.astype(bf16)


def attention_in_kernel(groups, chunks, me_ref, *refs):
    n = len(chunks)
    right_refs = refs[:groups]
    w_query_ref, w_key_ref, w_value_gate_ref, q_ref, g_ref = refs[groups : groups + 5]
    k_refs, v_refs = refs[groups + 5 : groups + 5 + n], refs[groups + 5 + n : groups + 5 + 2 * n]
    all_ref = refs[-1]
    channels = w_query_ref.shape[0]
    me = me_ref[0]
    tiles = all_ref.shape[1] // SUB
    for s in range(groups):
        d = lax.bitwise_xor(me, s)
        for place, (slab, tile) in single_places(q_ref.shape, right_refs[s].shape[1]).items():
            t, at = divmod(place, tiles)
            all_ref[d, at * SUB : (at + 1) * SUB, t * LANES : (t + 1) * LANES] = right_refs[s][slab, tile].astype(f32)
    own = all_ref[me].astype(bf16)
    q_ref[...] = jnp.dot(own, w_query_ref[...], preferred_element_type=f32).astype(bf16)
    g_ref[...] = sigmoid(jnp.dot(own, w_value_gate_ref[:, channels:], preferred_element_type=f32))
    first = 0
    for k in range(n):
        every = all_ref[:, first * SUB : (first + chunks[k]) * SUB].reshape(k_refs[k].shape).astype(bf16)
        k_refs[k][...] = jnp.dot(every, w_key_ref[...], preferred_element_type=f32).astype(bf16)
        v_refs[k][...] = jnp.dot(every, w_value_gate_ref[:, :channels], preferred_element_type=f32).astype(bf16)
        first += chunks[k]


def tail_kernel(sets, per_set, heads, slab, attends, me_ref, *refs):
    tri_refs = refs[:sets]
    pair_ref, gate_ref, w_tri_out_ref, w_in_ref, w_down_ref, w_bias_ref = refs[sets : sets + 6]
    if attends:
        new_ref, single_ref, bias_ref, w_rel_ref, wb_ref = refs[-5:]
    else:
        new_ref, bias_ref, w_rel_ref, wb_ref = refs[-4:]
    width = pair_ref.shape[-1]
    columns = math.prod(pair_ref.shape[1:-1])
    together = LANES // columns
    inner_width = w_down_ref.shape[0]
    me = me_ref[0]

    @pl.when(pl.program_id(0) == 0)
    def _():
        own_set = lax.rem(me, sets)
        for a in range(sets):
            w_rel_ref[a * per_set : (a + 1) * per_set] = w_tri_out_ref[lax.bitwise_xor(own_set, a)]
        wb_ref[...] = w_bias_ref[...].T

    low = first_half_lanes((per_set // 2, LANES))

    def sums_of(i):
        parts = []
        for r in tri_refs:
            if together == 1:
                parts.append(r[i].astype(f32))
            else:
                here, there = r[i].astype(f32), r[i + 1].astype(f32)
                parts.append(jnp.where(low, here, pltpu.roll(there, LANES // 2, 1)))
                parts.append(jnp.where(low, pltpu.roll(here, LANES // 2, 1), there))
        return jnp.concatenate(parts, axis=0)

    def rows(b, carry):
        i = b * slab * together
        tri = []
        for n in range(slab):
            tri.append(layer_norm(sums_of(i + n * together), 0).astype(bf16).T)
        tri = jnp.concatenate(tri, axis=0)
        tri_out = jnp.dot(tri, w_rel_ref[...], preferred_element_type=f32)
        here = pl.ds(i, slab * together)
        block = (slab * LANES, width)
        mid = pair_ref[here].reshape(block) + gate_ref[here].reshape(block) * tri_out
        trans = layer_norm(mid, 1).astype(bf16)
        gate_up = jnp.dot(trans, w_in_ref[...], preferred_element_type=f32)
        gate = gate_up[:, :inner_width]
        inner = (gate * sigmoid(gate) * gate_up[:, inner_width:]).astype(bf16)
        new = mid + jnp.dot(inner, w_down_ref[...], preferred_element_type=f32)
        new_ref[here] = new.reshape((slab * together,) + new_ref.shape[1:])
        normed = layer_norm(new, 1).astype(bf16)
        bias = lax.dot_general(wb_ref[...], normed, NT, preferred_element_type=f32)
        for n in range(slab):
            part = bias[:, n * LANES : (n + 1) * LANES]
            bias_ref[i + n * together] = part
            if together == 2:
                bias_ref[i + n * together + 1] = pltpu.roll(part, LANES // 2, 1)
        return carry

    lax.fori_loop(0, pair_ref.shape[0] // (slab * together), rows, 0)
    if attends:
        attention(heads, attends, refs[sets + 6 :], bias_ref, single_ref)


def attention(heads, n, refs, last_bias_ref, single_ref):
    q_ref, g_ref, w_out_ref = refs[:3]
    k_refs, v_refs, live_refs = refs[3 : 3 + n], refs[3 + n : 3 + 2 * n], refs[3 + 2 * n : 3 + 3 * n]
    bias_refs = [*refs[3 + 3 * n : 2 + 4 * n], last_bias_ref]
    row_count, channels = q_ref.shape
    head_size = channels // heads
    of_head = lax.broadcasted_iota(jnp.int32, (row_count, heads, channels), 1)
    lane = lax.broadcasted_iota(jnp.int32, (row_count, heads, channels), 2)
    mine = jnp.logical_and(lane >= of_head * head_size, lane < (of_head + 1) * head_size)
    spread = jnp.where(mine, jnp.broadcast_to(q_ref[...].astype(f32)[:, None, :], mine.shape), 0.0)
    spread = spread.reshape(row_count * heads, channels).astype(bf16)
    scores = []
    for k in range(n):
        part = lax.dot_general(spread, k_refs[k][...], NT, preferred_element_type=f32)
        bias = bias_refs[k][...].reshape(row_count * heads, LANES)[:, : part.shape[1]]
        part = part / jnp.sqrt(f32(head_size)) + bias
        scores.append(jnp.where(live_refs[k][...] > 0, part, f32(-1000000000.0)))
    row_max = functools.reduce(jnp.maximum, [jnp.max(x, axis=1, keepdims=True) for x in scores])
    weights = [jnp.exp(x - row_max) for x in scores]
    row_sum = sum(jnp.sum(x, axis=1, keepdims=True) for x in weights)
    attended = sum(
        jnp.dot((x / row_sum).astype(bf16), v[...], preferred_element_type=f32) for x, v in zip(weights, v_refs)
    )
    attended = jnp.sum(jnp.where(mine, attended.reshape(mine.shape), 0.0), axis=1)
    gated = (g_ref[...] * attended).astype(bf16)
    single_ref[...] = jnp.dot(gated, w_out_ref[...], preferred_element_type=f32)


def whole_block(shape):
    return pl.BlockSpec(shape, lambda *_: (0,) * len(shape))


def params():
    return pltpu.CompilerParams(dimension_semantics=("arbitrary",))


def anywhere(arrays):
    return [pl.BlockSpec(memory_space=pl.ANY)] * len(arrays)


def cost(flops):
    return pl.CostEstimate(flops=int(flops), bytes_accessed=4000000, transcendentals=0)


def exchange(x, groups, s):
    return x if s == 0 else lax.ppermute(x, "row", [(r, r ^ s) for r in range(groups)])


def chunk_tiles(tiles, groups):
    most = LANES // (groups * SUB)
    chunks = [most] * (tiles // most) if most else []
    return chunks + ([tiles % most] if most and tiles % most else [])


def fast_body(
    pair, single, token_mask, w_tri_proj, w_tri_gate, w_tri_out, w_trans_in, w_trans_out, w_bias, w_query, w_key, w_value_gate, w_out
):
    row_count, length, width = pair.shape
    groups = lax.axis_size("row")
    sets = groups // 2
    hidden = w_tri_out.shape[0]
    per_set = hidden // sets
    message = per_set * 3 // 2
    inner_width = w_trans_out.shape[0]
    heads = w_bias.shape[1]
    channels = single.shape[1]
    slabs = single_slabs(single.shape, chunk_tiles(row_count // SUB, groups)[0], message)
    full = length // LANES * LANES
    lanes = full + LANES
    tiles = row_count // SUB
    chunks = chunk_tiles(tiles, groups)
    starts = [sum(chunks[:k]) for k in range(len(chunks))]
    me = lax.axis_index("row").astype(jnp.int32).reshape(1)
    live = token_mask.astype(f32)
    sds = jax.ShapeDtypeStruct
    message_block = lambda n: pl.BlockSpec((n, 1, SUB, LANES), lambda g, *_: (0, g, 0, 0))
    edge_scratch = [pltpu.VMEM((SUB * (hidden + SUB), LANES), f32)] * 2 + [pltpu.VMEM((2 * hidden, width), bf16)]
    edge_flops = 2 * SUB * lanes * width * 2 * hidden

    def right_edges(k, after):
        at = starts[k]
        size = message + (0 if k else slabs)
        return pl.pallas_call(
            functools.partial(right_kernel, hidden, full, sets, row_count, at * SUB, 0 if k else chunks[0]),
            name="right",
            grid_spec=pltpu.PrefetchScalarGridSpec(
                num_scalar_prefetch=2,
                grid=(chunks[k],),
                in_specs=[
                    pl.BlockSpec((SUB, length, width), lambda g, *_: (at + g, 0, 0)),
                    whole_block(single.shape),
                    whole_block((length,)),
                    pl.BlockSpec((width, 2 * hidden), lambda *_: (0, 1)),
                ]
                + anywhere(after),
                out_specs=[message_block(size)] * sets,
                scratch_shapes=edge_scratch,
            ),
            out_shape=[sds((size, chunks[k], SUB, LANES), bf16)] * sets,
            compiler_params=params(),
            cost_estimate=cost(edge_flops * chunks[k]),
        )(me, token_mask, pair, single, token_mask, w_tri_proj, *after)

    def left_edges(after):
        return pl.pallas_call(
            functools.partial(left_kernel, hidden, full, sets, row_count),
            name="left",
            grid_spec=pltpu.PrefetchScalarGridSpec(
                num_scalar_prefetch=2,
                grid=(tiles,),
                in_specs=[
                    pl.BlockSpec((SUB, length, width), lambda g, *_: (g, 0, 0)),
                    whole_block((length,)),
                    pl.BlockSpec((width, 2 * hidden), lambda *_: (0, 0)),
                ]
                + anywhere(after),
                out_specs=[message_block(message)] * sets,
                scratch_shapes=edge_scratch,
            ),
            out_shape=[sds((message, tiles, SUB, LANES), bf16)] * sets,
            compiler_params=params(),
            cost_estimate=cost(edge_flops * tiles),
        )(me, token_mask, pair, token_mask, w_tri_proj, *after)

    right_in, left_in, after = [], None, []
    for k in range(len(chunks)):
        right = right_edges(k, after)
        right_in.append([exchange(right[s % sets], groups, s) for s in range(groups)])
        after = [right[0]]
        if left_in is None:
            left = left_edges(after)
            left_in = [exchange(left[s], groups, s) for s in range(sets)]
            after = [left[0]]

    gate_pair = pl.pallas_call(
        gate_kernel,
        name="gate",
        grid=(tiles,),
        in_specs=[pl.BlockSpec((SUB, length, width), lambda g: (g, 0, 0)), whole_block((width, width))] + anywhere(after),
        out_specs=pl.BlockSpec((SUB, length, width), lambda g: (g, 0, 0)),
        out_shape=sds(pair.shape, f32),
        compiler_params=params(),
        cost_estimate=cost(2 * row_count * length * width * width),
    )(pair, w_tri_gate, *after)

    tokens = [groups * n * SUB for n in chunks]
    queries, att_gate, *keys_values = pl.pallas_call(
        functools.partial(attention_in_kernel, groups, chunks),
        name="attention_in",
        grid_spec=pltpu.PrefetchScalarGridSpec(
            num_scalar_prefetch=1,
            grid=(1,),
            in_specs=[pl.BlockSpec((slabs, chunks[0], SUB, LANES), lambda *_: (message // slabs, 0, 0, 0))] * groups
            + [whole_block(w_query.shape), whole_block(w_key.shape), whole_block(w_value_gate.shape)],
            out_specs=[whole_block((row_count, channels))] * 2 + [whole_block((n, channels)) for n in tokens + tokens],
            scratch_shapes=[pltpu.VMEM((groups, row_count, channels), f32)],
        ),
        out_shape=[sds((row_count, channels), bf16), sds((row_count, channels), f32)]
        + [sds((n, channels), bf16) for n in tokens + tokens],
        compiler_params=params(),
        cost_estimate=cost(2 * length * channels * channels * 3),
    )(me, *right_in[0], w_query, w_key, w_value_gate)

    total = sets * row_count
    tri_in = []
    for k in range(len(chunks)):
        late = queries
        columns = groups * chunks[k] * SUB
        sums_shape = (row_count, per_set * columns // LANES, LANES)
        sums = pl.pallas_call(
            functools.partial(triangle_kernel, groups, sets, per_set),
            grid_spec=pltpu.PrefetchScalarGridSpec(
                num_scalar_prefetch=1,
                grid=(1,),
                in_specs=[whole_block((message, chunks[k], SUB, LANES))] * groups
                + [whole_block((message, tiles, SUB, LANES))] * sets
                + anywhere([late]),
                out_specs=[whole_block(sums_shape)] * sets,
                scratch_shapes=[
                    pltpu.VMEM((per_set, groups, chunks[k] * SUB, LANES), f32),
                    pltpu.VMEM((per_set // 2, groups, chunks[k] * SUB, LANES), f32),
                    pltpu.VMEM((per_set * (total + SUB), LANES), f32),
                ],
            ),
            out_shape=[sds(sums_shape, bf16)] * sets,
            compiler_params=params(),
            cost_estimate=cost(2 * per_set * total * lanes * LANES),
        )(me, *right_in[k], *left_in, late)
        tri_in.append([exchange(sums[a], groups, a) for a in range(sets)])

    tiled = (row_count, groups, tiles, SUB, width)
    pair_tiled, gate_tiled = pair.reshape(tiled), gate_pair.reshape(tiled)
    new, biases = None, []
    lives = [
        live.reshape(groups, tiles, SUB)[:, at : at + n].reshape(1, groups * n * SUB) for at, n in zip(starts, chunks)
    ]
    for k, n in enumerate(chunks):
        attends = len(chunks) if k == len(chunks) - 1 else 0
        columns = tokens[k]
        together = LANES // columns
        take = row_count if attends else SUB
        slab = take // together
        at = starts[k] // n
        part_rows = pl.BlockSpec((take, groups, n, SUB, width), lambda g, *_, at=at: (g, 0, at, 0, 0))
        operands = [*tri_in[k], pair_tiled, gate_tiled, w_tri_out.reshape(sets, per_set, width), w_trans_in, w_trans_out, w_bias]
        sums_block = (take,) + tri_in[k][0].shape[1:]
        in_specs = [pl.BlockSpec(sums_block, lambda g, *_: (g, 0, 0))] * sets + [part_rows, part_rows]
        if attends:
            operands += [queries, att_gate, w_out, *keys_values, *lives, *biases]
        in_specs += [whole_block(x.shape) for x in operands[sets + 2 :]]
        aliases = {}
        if new is not None:
            aliases = {1 + len(operands): 0}
            operands.append(new)
            in_specs += anywhere([new])
        bias_shape = (row_count, heads, LANES)
        weights = [pltpu.VMEM((hidden, width), bf16), pltpu.VMEM((heads, width), bf16)]
        new, last = pl.pallas_call(
            functools.partial(tail_kernel, sets, per_set, heads, slab, attends),
            grid_spec=pltpu.PrefetchScalarGridSpec(
                num_scalar_prefetch=1,
                grid=(row_count // take,),
                in_specs=in_specs,
                out_specs=[
                    part_rows,
                    whole_block(single.shape) if attends else pl.BlockSpec((SUB, heads, LANES), lambda g, *_: (g, 0, 0)),
                ],
                scratch_shapes=([pltpu.VMEM(bias_shape, f32)] if attends else []) + weights,
            ),
            out_shape=[sds(tiled, f32), sds(single.shape if attends else bias_shape, f32)],
            input_output_aliases=aliases,
            compiler_params=params(),
            cost_estimate=cost(2 * row_count * columns * width * (hidden + 3 * inner_width)),
        )(me, *operands)
        biases.append(last)
    return new.reshape(pair.shape), last


def triangle(pieces):
    left_op, right_op = pieces
    return jnp.einsum("gcik,gcjk->gcij", left_op, right_op, preferred_element_type=jnp.float32)


def plain_body(
    pair,
    single,
    token_mask,
    w_tri_proj,
    w_tri_gate,
    w_tri_out,
    w_trans_in,
    w_trans_out,
    w_bias,
    w_query,
    w_key,
    w_value_gate,
    w_out,
):
    row_count, length, pair_width = pair.shape
    groups = lax.axis_size("row")
    hidden = w_tri_out.shape[0]
    per_dev = hidden // groups
    inner_width = w_trans_out.shape[0]
    head_count = w_bias.shape[1]
    channels = single.shape[1]
    head_size = channels // head_count
    row_start = lax.axis_index("row") * row_count
    live_all = token_mask.astype(jnp.float32)
    own_live = lax.dynamic_slice_in_dim(live_all, row_start, row_count)
    pair_live = own_live[:, None] * live_all[None, :]
    normed = layer_norm(pair, 2).astype(jnp.bfloat16)

    def operand(offset):
        weights_two = w_tri_proj[:, offset * hidden : (offset + 2) * hidden].reshape(
            pair_width, 2, groups, per_dev
        )
        projected = jnp.einsum(
            "ikd,dsgc->sgcik", normed, weights_two, preferred_element_type=jnp.float32
        )
        return (jax.nn.sigmoid(projected[1]) * projected[0] * pair_live).astype(jnp.bfloat16)

    left_edge = operand(0)
    right_edge = operand(2)
    product = triangle(
        (
            lax.all_to_all(left_edge, "row", split_axis=0, concat_axis=2, tiled=True),
            lax.all_to_all(right_edge, "row", split_axis=0, concat_axis=2, tiled=True),
        )
    )
    returned = lax.all_to_all(
        product.astype(jnp.bfloat16), "row", split_axis=2, concat_axis=0, tiled=True
    ).astype(product.dtype)
    summed = returned.reshape(hidden, row_count, length)
    triangle_normed = layer_norm(summed, 0).astype(jnp.bfloat16)
    tri_out = jnp.einsum(
        "cij,cd->ijd", triangle_normed, w_tri_out, preferred_element_type=jnp.float32
    )
    gate_pair = jax.nn.sigmoid(
        jnp.einsum("ijc,cd->ijd", normed, w_tri_gate, preferred_element_type=jnp.float32)
    )
    pair_mid = pair + gate_pair * tri_out
    block_rows = math.gcd(row_count, 8)

    def transition(row_slab):
        trans_normed = layer_norm(row_slab, 2).astype(jnp.bfloat16)
        gate_up = jnp.einsum(
            "ijc,cf->ijf", trans_normed, w_trans_in, preferred_element_type=jnp.float32
        )
        inner_act = (jax.nn.silu(gate_up[..., :inner_width]) * gate_up[..., inner_width:]).astype(
            jnp.bfloat16
        )
        return row_slab + jnp.einsum(
            "ijf,fc->ijc", inner_act, w_trans_out, preferred_element_type=jnp.float32
        )

    pair_new = lax.map(
        transition, pair_mid.reshape(row_count // block_rows, block_rows, length, pair_width)
    ).reshape(row_count, length, pair_width)
    bias_normed = layer_norm(pair_new, 2).astype(jnp.bfloat16)
    bias = jnp.einsum("ijc,ch->hij", bias_normed, w_bias, preferred_element_type=jnp.float32)
    single_normed = layer_norm(single, 1).astype(jnp.bfloat16)
    queries = jnp.dot(single_normed, w_query, preferred_element_type=jnp.float32).astype(
        jnp.bfloat16
    )
    att_gate = jax.nn.sigmoid(
        jnp.dot(single_normed, w_value_gate[:, channels:], preferred_element_type=jnp.float32)
    )
    normed_all = lax.all_gather(single_normed, "row", axis=0, tiled=True)
    keys_all = jnp.dot(normed_all, w_key, preferred_element_type=jnp.float32).astype(jnp.bfloat16)
    values_all = jnp.dot(
        normed_all, w_value_gate[:, :channels], preferred_element_type=jnp.float32
    ).astype(jnp.bfloat16)
    query_heads = queries.reshape(row_count, head_count, head_size)
    key_heads = keys_all.reshape(length, head_count, head_size)
    value_heads = values_all.reshape(length, head_count, head_size)
    scores = (
        jnp.einsum("ihd,jhd->hij", query_heads, key_heads, preferred_element_type=jnp.float32)
        / jnp.sqrt(jnp.float32(head_size))
        + bias
    )
    scores = jnp.where(live_all[None, None, :] > 0, scores, jnp.float32(-1000000000.0))
    row_max = jnp.max(scores, axis=2, keepdims=True)
    weights = jnp.exp(scores - row_max)
    weights = weights / jnp.sum(weights, axis=2, keepdims=True)
    probs = weights.astype(jnp.bfloat16)
    attended = jnp.einsum(
        "hij,jhd->ihd", probs, value_heads, preferred_element_type=jnp.float32
    ).reshape(row_count, channels)
    gated = (att_gate * attended).astype(jnp.bfloat16)
    single_update = jnp.dot(gated, w_out, preferred_element_type=jnp.float32)
    return (pair_new, single_update)


def body(*arrays):
    pair, single, w_tri_out = arrays[0], arrays[1], arrays[5]
    row_count, length, _ = pair.shape
    groups = lax.axis_size("row")
    hidden = w_tri_out.shape[0]
    sets = groups // 2
    packs = (
        groups >= 4
        and groups & (groups - 1) == 0
        and hidden % (32 * sets) == 0
        and (length % LANES) * 2 == LANES
        and length // LANES == 1
        and row_count % SUB == 0
        and single.shape[1] % LANES == 0
        and all(groups * n * SUB in (LANES, LANES // 2) for n in chunk_tiles(row_count // SUB, groups))
        and bool(chunk_tiles(row_count // SUB, groups))
    )
    if not packs:
        return plain_body(*arrays)
    return fast_body(*arrays)


def solution(mesh):
    in_specs = (
        P(("crop", "row"), None, None),
        P(("crop", "row"), None),
        P("crop"),
        P(),
        P(),
        P(),
        P(),
        P(),
        P(),
        P(),
        P(),
        P(),
        P(),
    )
    out_specs = (P(("crop", "row"), None, None), P(("crop", "row"), None))
    return jax.shard_map(body, mesh=mesh, in_specs=in_specs, out_specs=out_specs, check_vma=False)
```

```python
import functools
import math

import jax
import jax.numpy as jnp
from jax import lax
from jax.experimental import pallas as pl
from jax.experimental.pallas import tpu as pltpu
from jax.sharding import PartitionSpec as P


epsilon = 1e-05
LANES = 128
SUB = 8
f32 = jnp.float32
bf16 = jnp.bfloat16
NT = (((1,), (1,)), ((), ()))


def layer_norm(values_in, along):
    average = jnp.mean(values_in, axis=along, keepdims=True)
    centered = values_in - average
    spread = jnp.mean(centered * centered, axis=along, keepdims=True)
    return centered * lax.rsqrt(spread + epsilon)


def sigmoid(x):
    return 0.5 * jnp.tanh(0.5 * x) + 0.5


def repeat_rest(x, full):
    return jnp.concatenate([x, x[full:]], axis=0)


def first_half_lanes(shape):
    return lax.broadcasted_iota(jnp.int32, shape, len(shape) - 1) < LANES // 2


def edges_to_messages(me_ref, mask_ref, live_ref, wt_ref, rows_of, head_ref, rest_ref, out_refs, first, hidden, full):
    sets = len(out_refs)
    per_set = hidden // sets
    pairs = per_set // 2
    stride = hidden + SUB
    own_set = lax.rem(me_ref[0], sets)
    tokens = live_ref[...].astype(f32).reshape(1, live_ref.shape[0])
    tokens = jnp.concatenate([tokens, tokens[:, full:]], axis=1)
    for j in range(SUB):
        x = repeat_rest(rows_of(j), full)
        projected = lax.dot_general(wt_ref[...], x, NT, preferred_element_type=f32)
        live = tokens * mask_ref[first + j].astype(f32)
        edge = sigmoid(projected[hidden:]) * projected[:hidden] * live
        for s in range(sets):
            q = lax.bitwise_xor(own_set, s)
            at = pl.multiple_of(j * stride + q * per_set, SUB)
            part = edge[s * per_set : (s + 1) * per_set]
            head_ref[pl.ds(at, per_set), :] = part[:, :LANES]
            rest_ref[pl.ds(at, per_set), :] = part[:, LANES:]
    step = pl.program_id(0)
    low = first_half_lanes((SUB, LANES))
    for q in range(sets):
        for c in range(pairs):
            a = pl.ds(q * per_set + c, SUB, stride=stride)
            b = pl.ds(q * per_set + pairs + c, SUB, stride=stride)
            out_refs[q][c, step] = head_ref[a, :].astype(bf16)
            out_refs[q][pairs + c, step] = head_ref[b, :].astype(bf16)
            out_refs[q][per_set + c, step] = jnp.where(low, rest_ref[a, :], rest_ref[b, :]).astype(bf16)


def single_places(shape, tiles):
    pieces = shape[1] // LANES * (shape[0] // SUB)
    return {n: divmod(n, tiles) for n in range(pieces)}


def single_slabs(shape, tiles, message):
    least = -(-(shape[1] // LANES * (shape[0] // SUB)) // tiles)
    return next(n for n in range(least, message + 1) if message % n == 0)


def right_kernel(hidden, full, sets, row_count, offset, single_tiles, me_ref, mask_ref, pair_ref, single_ref, live_ref, w_ref, *rest):
    out_refs = rest[-3 - sets : -3]
    head_ref, rest_ref, wt_ref = rest[-3:]

    @pl.when(pl.program_id(0) == 0)
    def _():
        wt_ref[...] = w_ref[...].T

    first = me_ref[0] * row_count + offset + pl.program_id(0) * SUB
    at = 0 if single_tiles else offset + pl.program_id(0) * SUB
    rows_of = lambda j: layer_norm(pair_ref[at + j], 1).astype(bf16)
    edges_to_messages(me_ref, mask_ref, live_ref, wt_ref, rows_of, head_ref, rest_ref, out_refs, first, hidden, full)
    if single_tiles:
        single_normed = layer_norm(single_ref[...], 1)
        base = hidden // sets * 3 // 2
        for g in range(single_tiles):

            @pl.when(pl.program_id(0) == g)
            def _():
                for n, (slab, tile) in single_places(single_ref.shape, single_tiles).items():
                    if tile == g:
                        t, at = divmod(n, row_count // SUB)
                        part = single_normed[at * SUB : (at + 1) * SUB, t * LANES : (t + 1) * LANES].astype(bf16)
                        for q in range(sets):
                            out_refs[q][base + slab, tile] = part


def left_kernel(hidden, full, sets, row_count, me_ref, mask_ref, pair_ref, live_ref, w_ref, *rest):
    out_refs = rest[-3 - sets : -3]
    head_ref, rest_ref, wt_ref = rest[-3:]

    @pl.when(pl.program_id(0) == 0)
    def _():
        wt_ref[...] = w_ref[...].T

    first = me_ref[0] * row_count + pl.program_id(0) * SUB
    rows_of = lambda j: layer_norm(pair_ref[pl.program_id(0) * SUB + j], 1).astype(bf16)
    edges_to_messages(me_ref, mask_ref, live_ref, wt_ref, rows_of, head_ref, rest_ref, out_refs, first, hidden, full)


def gate_kernel(pair_ref, w_gate_ref, _, gate_ref):
    width = pair_ref.shape[2]

    def rows(g, carry):
        here = pl.ds(g * SUB, SUB)
        block = pair_ref[here]
        x = layer_norm(block.reshape(SUB * block.shape[1], width), 1).astype(bf16)
        gate_ref[here] = sigmoid(jnp.dot(x, w_gate_ref[...], preferred_element_type=f32)).reshape(block.shape)
        return carry

    lax.fori_loop(0, pair_ref.shape[0] // SUB, rows, 0)


def plain_rows(block):
    wide = block.astype(f32)
    return wide.reshape(wide.shape[0] * wide.shape[1], wide.shape[2])


def triangle_kernel(groups, sets, per_set, me_ref, *refs):
    right_refs, left_refs = refs[:groups], refs[groups : groups + sets]
    out_refs = refs[-sets - 3 : -3]
    head_ref, rest_ref, sums_ref = refs[-3:]
    pairs = per_set // 2
    rows = left_refs[0].shape[1] * SUB
    here = right_refs[0].shape[1] * SUB
    columns = groups * here
    me = me_ref[0]
    total = sets * rows
    stride = total + SUB
    low = first_half_lanes((total, LANES))
    fill = lambda x: x if columns == LANES else jnp.concatenate([x, x], axis=0)
    for s in range(groups):
        d = lax.bitwise_xor(me, s)
        wide = right_refs[s][: per_set + pairs].astype(f32).reshape(per_set + pairs, here, LANES)
        head_ref[:, d] = wide[:per_set]
        rest_ref[:, d] = wide[per_set:]
    for c in range(pairs):
        right_rest = fill(rest_ref[c].reshape(columns, LANES)).astype(bf16)
        left_rest = jnp.concatenate([plain_rows(r[per_set + c]) for r in left_refs], axis=0)
        for p in range(2):
            channel = p * pairs + c
            right = fill(head_ref[channel].reshape(columns, LANES)).astype(bf16)
            left = jnp.concatenate([plain_rows(r[channel]) for r in left_refs], axis=0).astype(bf16)
            kept = jnp.where(low if p == 0 else jnp.logical_not(low), left_rest, 0.0).astype(bf16)
            sums_ref[channel * stride : channel * stride + total, :] = lax.dot_general(
                jnp.concatenate([left, kept], axis=1),
                jnp.concatenate([right, right_rest], axis=1),
                NT,
                preferred_element_type=f32,
            )
    low_half = first_half_lanes((pairs, LANES))
    for a in range(sets):
        for i in range(rows):
            x = sums_ref[pl.ds(a * rows + i, per_set, stride=stride), :]
            if columns < LANES:
                x = jnp.where(low_half, x[:pairs], x[pairs:])
            out_refs[a][i] = x.astype(bf16)


def attention_in_kernel(groups, chunks, message, me_ref, *refs):
    n = len(chunks)
    right_refs = refs[:groups]
    w_query_ref, w_key_ref, w_value_gate_ref, q_ref, g_ref = refs[groups : groups + 5]
    k_refs, v_refs = refs[groups + 5 : groups + 5 + n], refs[groups + 5 + n : groups + 5 + 2 * n]
    all_ref = refs[-1]
    channels = w_query_ref.shape[0]
    me = me_ref[0]
    tiles = all_ref.shape[1] // SUB
    for s in range(groups):
        d = lax.bitwise_xor(me, s)
        for place, (slab, tile) in single_places(q_ref.shape, right_refs[s].shape[1]).items():
            t, at = divmod(place, tiles)
            all_ref[d, at * SUB : (at + 1) * SUB, t * LANES : (t + 1) * LANES] = right_refs[s][
                message + slab, tile
            ].astype(f32)
    own = all_ref[me].astype(bf16)
    q_ref[...] = jnp.dot(own, w_query_ref[...], preferred_element_type=f32).astype(bf16)
    g_ref[...] = sigmoid(jnp.dot(own, w_value_gate_ref[:, channels:], preferred_element_type=f32))
    first = 0
    for k in range(n):
        every = all_ref[:, first * SUB : (first + chunks[k]) * SUB].reshape(k_refs[k].shape).astype(bf16)
        k_refs[k][...] = jnp.dot(every, w_key_ref[...], preferred_element_type=f32).astype(bf16)
        v_refs[k][...] = jnp.dot(every, w_value_gate_ref[:, :channels], preferred_element_type=f32).astype(bf16)
        first += chunks[k]


def tail_kernel(sets, per_set, heads, slab, attends, first, me_ref, *refs):
    tri_refs = refs[:sets]
    pair_ref, gate_ref, w_tri_out_ref, w_in_ref, w_down_ref, w_bias_ref = refs[sets : sets + 6]
    if attends:
        new_ref, single_ref, bias_ref, w_rel_ref, w_half_ref = refs[-5:]
    else:
        new_ref, bias_ref, w_rel_ref, w_half_ref = refs[-4:]
    width = pair_ref.shape[-1]
    columns = math.prod(new_ref.shape[1:-1])
    part = slice(first, first + new_ref.shape[2])
    together = LANES // columns
    inner_width = w_down_ref.shape[0]
    me = me_ref[0]

    @pl.when(pl.program_id(0) == 0)
    def _():
        own_set = lax.rem(me, sets)
        for a in range(sets):
            w_rel_ref[a * per_set : (a + 1) * per_set] = w_tri_out_ref[lax.bitwise_xor(own_set, a)]
        w_half_ref[:, :inner_width] = w_in_ref[:, :inner_width] * 0.5
        w_half_ref[:, inner_width:] = w_in_ref[:, inner_width:]

    low = first_half_lanes((per_set // 2, LANES))
    start = pl.program_id(0) * new_ref.shape[0]

    def sums_of(i):
        parts = []
        for r in tri_refs:
            if together == 1:
                parts.append(r[i].astype(f32))
            else:
                here, there = r[i].astype(f32), r[i + 1].astype(f32)
                parts.append(jnp.where(low, here, pltpu.roll(there, LANES // 2, 1)))
                parts.append(jnp.where(low, pltpu.roll(here, LANES // 2, 1), there))
        return jnp.concatenate(parts, axis=0)

    def rows(b, carry):
        i = b * slab * together
        tri = []
        for n in range(slab):
            tri.append(layer_norm(sums_of(start + i + n * together), 0).astype(bf16).T)
        tri = jnp.concatenate(tri, axis=0)
        tri_out = jnp.dot(tri, w_rel_ref[...], preferred_element_type=f32)
        here, there = pl.ds(i, slab * together), pl.ds(start + i, slab * together)
        block = (slab * LANES, width)
        mid = pair_ref[there, :, part].reshape(block) + gate_ref[there, :, part].reshape(block) * tri_out
        trans = layer_norm(mid, 1).astype(bf16)
        gate_up = jnp.dot(trans, w_half_ref[...], preferred_element_type=f32)
        half = gate_up[:, :inner_width]
        scaled = half * gate_up[:, inner_width:]
        inner = (scaled + scaled * jnp.tanh(half)).astype(bf16)
        new = mid + jnp.dot(inner, w_down_ref[...], preferred_element_type=f32)
        new_ref[here] = new.reshape((slab * together,) + new_ref.shape[1:])
        normed = layer_norm(new, 1).astype(bf16)
        bias = lax.dot_general(w_bias_ref[...], normed, NT, preferred_element_type=f32)
        for n in range(slab):
            lane_tile = bias[:, n * LANES : (n + 1) * LANES]
            bias_ref[i + n * together] = lane_tile
            if together == 2:
                bias_ref[i + n * together + 1] = pltpu.roll(lane_tile, LANES // 2, 1)
        return carry

    lax.fori_loop(0, new_ref.shape[0] // (slab * together), rows, 0)
    if attends:
        attention(heads, attends, pair_ref.shape[1], refs[sets + 6 :], bias_ref, single_ref)


def attention(heads, n, groups, refs, last_bias_ref, single_ref):
    q_ref, g_ref, w_out_ref, mask_ref = refs[:4]
    k_refs, v_refs = refs[4 : 4 + n], refs[4 + n : 4 + 2 * n]
    bias_refs = [*refs[4 + 2 * n : 3 + 3 * n], last_bias_ref]
    count = jnp.sum(mask_ref[...].astype(f32).reshape(1, mask_ref.shape[0]), axis=1, keepdims=True)
    row_count, channels = q_ref.shape
    head_size = channels // heads
    of_head = lax.broadcasted_iota(jnp.int32, (row_count, heads, channels), 1)
    lane = lax.broadcasted_iota(jnp.int32, (row_count, heads, channels), 2)
    mine = jnp.logical_and(lane >= of_head * head_size, lane < (of_head + 1) * head_size)
    spread = jnp.where(mine, jnp.broadcast_to(q_ref[...].astype(f32)[:, None, :], mine.shape), 0.0)
    spread = spread.reshape(row_count * heads, channels).astype(bf16)
    scores, first = [], 0
    for k in range(n):
        part = lax.dot_general(spread, k_refs[k][...], NT, preferred_element_type=f32)
        bias = bias_refs[k][...].reshape(row_count * heads, LANES)[:, : part.shape[1]]
        part = part / jnp.sqrt(f32(head_size)) + bias
        column = lax.broadcasted_iota(jnp.int32, (1, part.shape[1]), 1)
        size = part.shape[1] // groups
        token = column // size * row_count + first + column % size
        first += size
        scores.append(jnp.where(token.astype(f32) < count, part, f32(-1000000000.0)))
    row_max = functools.reduce(jnp.maximum, [jnp.max(x, axis=1, keepdims=True) for x in scores])
    weights = [jnp.exp(x - row_max) for x in scores]
    row_sum = sum(jnp.sum(x, axis=1, keepdims=True) for x in weights)
    attended = sum(
        jnp.dot((x / row_sum).astype(bf16), v[...], preferred_element_type=f32) for x, v in zip(weights, v_refs)
    )
    attended = jnp.sum(jnp.where(mine, attended.reshape(mine.shape), 0.0), axis=1)
    gated = (g_ref[...] * attended).astype(bf16)
    single_ref[...] = jnp.dot(gated, w_out_ref[...], preferred_element_type=f32)


def whole_block(shape):
    return pl.BlockSpec(shape, lambda *_: (0,) * len(shape))


def params(**more):
    return pltpu.CompilerParams(dimension_semantics=("arbitrary",), **more)


def arrived(arrays):
    return [pltpu.with_memory_space_constraint(x, pltpu.VMEM) for x in arrays]


def kept(arrays):
    return [pltpu.with_memory_space_constraint(x, pltpu.HBM) for x in arrays]


def in_vmem(arrays):
    return [pl.BlockSpec(memory_space=pltpu.VMEM)] * len(arrays)


def anywhere(arrays):
    return [pl.BlockSpec(memory_space=pl.ANY)] * len(arrays)


def cost(flops):
    return pl.CostEstimate(flops=int(flops), bytes_accessed=4000000, transcendentals=0)


def exchange(x, groups, s):
    return x if s == 0 else lax.ppermute(x, "row", [(r, r ^ s) for r in range(groups)])


def chunk_tiles(tiles, groups):
    most = LANES // (groups * SUB)
    chunks = [most] * (tiles // most) if most else []
    return chunks + ([tiles % most] if most and tiles % most else [])


def fast_body(
    pair, single, token_mask, w_tri_proj, w_tri_gate, w_tri_out, w_trans_in, w_trans_out, w_bias, w_query, w_key, w_value_gate, w_out
):
    row_count, length, width = pair.shape
    groups = lax.axis_size("row")
    sets = groups // 2
    hidden = w_tri_out.shape[0]
    per_set = hidden // sets
    message = per_set * 3 // 2
    inner_width = w_trans_out.shape[0]
    heads = w_bias.shape[1]
    channels = single.shape[1]
    slabs = single_slabs(single.shape, chunk_tiles(row_count // SUB, groups)[0], message)
    full = length // LANES * LANES
    lanes = full + LANES
    tiles = row_count // SUB
    chunks = chunk_tiles(tiles, groups)
    starts = [sum(chunks[:k]) for k in range(len(chunks))]
    me = lax.axis_index("row").astype(jnp.int32).reshape(1)
    (near,) = arrived([pair])
    sds = jax.ShapeDtypeStruct
    edge_scratch = [pltpu.VMEM((SUB * (hidden + SUB), LANES), f32)] * 2 + [pltpu.VMEM((2 * hidden, width), bf16)]
    edge_flops = 2 * SUB * lanes * width * 2 * hidden

    def right_edges(k, after):
        at = starts[k]
        size = message + (0 if k else slabs)
        return pl.pallas_call(
            functools.partial(right_kernel, hidden, full, sets, row_count, at * SUB, 0 if k else chunks[0]),
            name="right",
            grid_spec=pltpu.PrefetchScalarGridSpec(
                num_scalar_prefetch=2,
                grid=(chunks[k],),
                in_specs=[
                    *(in_vmem([near]) if k else [pl.BlockSpec((SUB, length, width), lambda g, *_: (g, 0, 0))]),
                    whole_block(single.shape),
                    whole_block((length,)),
                    pl.BlockSpec((width, 2 * hidden), lambda *_: (0, 1)),
                ]
                + anywhere(after),
                out_specs=in_vmem([None] * sets),
                scratch_shapes=edge_scratch,
            ),
            out_shape=[sds((size, chunks[k], SUB, LANES), bf16)] * sets,
            compiler_params=params(vmem_limit_bytes=24 * 2**20),
            cost_estimate=cost(edge_flops * chunks[k]),
        )(me, token_mask, *([near, single, token_mask, w_tri_proj] if k else kept([pair, single, token_mask, w_tri_proj])), *after)

    def left_edges(after):
        return pl.pallas_call(
            functools.partial(left_kernel, hidden, full, sets, row_count),
            name="left",
            grid_spec=pltpu.PrefetchScalarGridSpec(
                num_scalar_prefetch=2,
                grid=(tiles,),
                in_specs=[
                    *in_vmem([near]),
                    whole_block((length,)),
                    pl.BlockSpec((width, 2 * hidden), lambda *_: (0, 0)),
                ]
                + anywhere(after),
                out_specs=in_vmem([None] * sets),
                scratch_shapes=edge_scratch,
            ),
            out_shape=[sds((message, tiles, SUB, LANES), bf16)] * sets,
            compiler_params=params(vmem_limit_bytes=24 * 2**20),
            cost_estimate=cost(edge_flops * tiles),
        )(me, token_mask, near, token_mask, w_tri_proj, *after)

    right_in, left_in, after = [], None, []
    for k in range(len(chunks)):
        right = right_edges(k, after)
        right_in.append([exchange(right[s % sets], groups, s) for s in range(groups)])
        after = [right[0]]
        if left_in is None:
            left = left_edges(after)
            left_in = [exchange(left[s], groups, s) for s in range(sets)]
            after = [left[0]]

    gate_pair = pl.pallas_call(
        gate_kernel,
        name="gate",
        in_specs=in_vmem([near, w_tri_gate]) + anywhere(after),
        out_specs=in_vmem([None])[0],
        out_shape=sds(pair.shape, f32),
        compiler_params=pltpu.CompilerParams(vmem_limit_bytes=16 * 2**20),
        cost_estimate=cost(2 * row_count * length * width * width),
    )(near, w_tri_gate, *after)

    tokens = [groups * n * SUB for n in chunks]
    queries, att_gate, *keys_values = pl.pallas_call(
        functools.partial(attention_in_kernel, groups, chunks, message),
        name="attention_in",
        grid_spec=pltpu.PrefetchScalarGridSpec(
            num_scalar_prefetch=1,
            grid=(1,),
            in_specs=in_vmem(right_in[0])
            + [whole_block(w_query.shape), whole_block(w_key.shape), whole_block(w_value_gate.shape)],
            out_specs=[whole_block((row_count, channels))] * 2 + [whole_block((n, channels)) for n in tokens + tokens],
            scratch_shapes=[pltpu.VMEM((groups, row_count, channels), f32)],
        ),
        out_shape=[sds((row_count, channels), bf16), sds((row_count, channels), f32)]
        + [sds((n, channels), bf16) for n in tokens + tokens],
        compiler_params=params(vmem_limit_bytes=16 * 2**20),
        cost_estimate=cost(2 * length * channels * channels * 3),
    )(me, *arrived(right_in[0]), w_query, w_key, w_value_gate)

    total = sets * row_count
    tri_in = []
    for k in range(len(chunks)):
        late = queries
        columns = groups * chunks[k] * SUB
        sums_shape = (row_count, per_set * columns // LANES, LANES)
        sums = pl.pallas_call(
            functools.partial(triangle_kernel, groups, sets, per_set),
            grid_spec=pltpu.PrefetchScalarGridSpec(
                num_scalar_prefetch=1,
                grid=(1,),
                in_specs=in_vmem(right_in[k] + left_in) + anywhere([late]),
                out_specs=[whole_block(sums_shape)] * sets,
                scratch_shapes=[
                    pltpu.VMEM((per_set, groups, chunks[k] * SUB, LANES), f32),
                    pltpu.VMEM((per_set // 2, groups, chunks[k] * SUB, LANES), f32),
                    pltpu.VMEM((per_set * (total + SUB), LANES), f32),
                ],
            ),
            out_shape=[sds(sums_shape, bf16)] * sets,
            compiler_params=params(vmem_limit_bytes=24 * 2**20),
            cost_estimate=cost(2 * per_set * total * lanes * LANES),
        )(me, *arrived(right_in[k] + left_in), late)
        tri_in.append([exchange(sums[a], groups, a) for a in range(sets)])

    tiled = (row_count, groups, tiles, SUB, width)
    pair_tiled, gate_tiled = arrived([pair.reshape(tiled), gate_pair.reshape(tiled)])
    new, biases = None, []
    for k, n in enumerate(chunks):
        attends = len(chunks) if k == len(chunks) - 1 else 0
        columns = tokens[k]
        together = LANES // columns
        take = row_count if attends else SUB
        slab = take // together
        at = starts[k] // n
        part_rows = pl.BlockSpec((take, groups, n, SUB, width), lambda g, *_, at=at: (g, 0, at, 0, 0))
        operands = [*arrived(tri_in[k]), pair_tiled, gate_tiled, w_tri_out.reshape(sets, per_set, width), w_trans_in, w_trans_out, w_bias.T]
        in_specs = in_vmem(operands[: sets + 2])
        if attends:
            operands += [queries, att_gate, w_out, token_mask, *keys_values, *biases]
        in_specs += [whole_block(x.shape) for x in operands[sets + 2 :]]
        aliases = {}
        if new is not None:
            aliases = {1 + len(operands): 0}
            operands.append(new)
            in_specs += anywhere([new])
        bias_shape = (row_count, heads, LANES)
        weights = [pltpu.VMEM((hidden, width), bf16), pltpu.VMEM(w_trans_in.shape, bf16)]
        new, last = pl.pallas_call(
            functools.partial(tail_kernel, sets, per_set, heads, slab, attends, starts[k]),
            grid_spec=pltpu.PrefetchScalarGridSpec(
                num_scalar_prefetch=1,
                grid=(row_count // take,),
                in_specs=in_specs,
                out_specs=[
                    part_rows,
                    whole_block(single.shape) if attends else pl.BlockSpec((SUB, heads, LANES), lambda g, *_: (g, 0, 0)),
                ],
                scratch_shapes=([pltpu.VMEM(bias_shape, f32)] if attends else []) + weights,
            ),
            out_shape=[sds(tiled, f32), sds(single.shape if attends else bias_shape, f32)],
            input_output_aliases=aliases,
            compiler_params=params(vmem_limit_bytes=32 * 2**20),
            cost_estimate=cost(2 * row_count * columns * width * (hidden + 3 * inner_width)),
        )(me, *operands)
        biases.append(last)
    return new.reshape(pair.shape), last


def triangle(pieces):
    left_op, right_op = pieces
    return jnp.einsum("gcik,gcjk->gcij", left_op, right_op, preferred_element_type=jnp.float32)


def plain_body(
    pair,
    single,
    token_mask,
    w_tri_proj,
    w_tri_gate,
    w_tri_out,
    w_trans_in,
    w_trans_out,
    w_bias,
    w_query,
    w_key,
    w_value_gate,
    w_out,
):
    row_count, length, pair_width = pair.shape
    groups = lax.axis_size("row")
    hidden = w_tri_out.shape[0]
    per_dev = hidden // groups
    inner_width = w_trans_out.shape[0]
    head_count = w_bias.shape[1]
    channels = single.shape[1]
    head_size = channels // head_count
    row_start = lax.axis_index("row") * row_count
    live_all = token_mask.astype(jnp.float32)
    own_live = lax.dynamic_slice_in_dim(live_all, row_start, row_count)
    pair_live = own_live[:, None] * live_all[None, :]
    normed = layer_norm(pair, 2).astype(jnp.bfloat16)

    def operand(offset):
        weights_two = w_tri_proj[:, offset * hidden : (offset + 2) * hidden].reshape(
            pair_width, 2, groups, per_dev
        )
        projected = jnp.einsum(
            "ikd,dsgc->sgcik", normed, weights_two, preferred_element_type=jnp.float32
        )
        return (jax.nn.sigmoid(projected[1]) * projected[0] * pair_live).astype(jnp.bfloat16)

    left_edge = operand(0)
    right_edge = operand(2)
    product = triangle(
        (
            lax.all_to_all(left_edge, "row", split_axis=0, concat_axis=2, tiled=True),
            lax.all_to_all(right_edge, "row", split_axis=0, concat_axis=2, tiled=True),
        )
    )
    returned = lax.all_to_all(
        product.astype(jnp.bfloat16), "row", split_axis=2, concat_axis=0, tiled=True
    ).astype(product.dtype)
    summed = returned.reshape(hidden, row_count, length)
    triangle_normed = layer_norm(summed, 0).astype(jnp.bfloat16)
    tri_out = jnp.einsum(
        "cij,cd->ijd", triangle_normed, w_tri_out, preferred_element_type=jnp.float32
    )
    gate_pair = jax.nn.sigmoid(
        jnp.einsum("ijc,cd->ijd", normed, w_tri_gate, preferred_element_type=jnp.float32)
    )
    pair_mid = pair + gate_pair * tri_out
    block_rows = math.gcd(row_count, 8)

    def transition(row_slab):
        trans_normed = layer_norm(row_slab, 2).astype(jnp.bfloat16)
        gate_up = jnp.einsum(
            "ijc,cf->ijf", trans_normed, w_trans_in, preferred_element_type=jnp.float32
        )
        inner_act = (jax.nn.silu(gate_up[..., :inner_width]) * gate_up[..., inner_width:]).astype(
            jnp.bfloat16
        )
        return row_slab + jnp.einsum(
            "ijf,fc->ijc", inner_act, w_trans_out, preferred_element_type=jnp.float32
        )

    pair_new = lax.map(
        transition, pair_mid.reshape(row_count // block_rows, block_rows, length, pair_width)
    ).reshape(row_count, length, pair_width)
    bias_normed = layer_norm(pair_new, 2).astype(jnp.bfloat16)
    bias = jnp.einsum("ijc,ch->hij", bias_normed, w_bias, preferred_element_type=jnp.float32)
    single_normed = layer_norm(single, 1).astype(jnp.bfloat16)
    queries = jnp.dot(single_normed, w_query, preferred_element_type=jnp.float32).astype(
        jnp.bfloat16
    )
    att_gate = jax.nn.sigmoid(
        jnp.dot(single_normed, w_value_gate[:, channels:], preferred_element_type=jnp.float32)
    )
    normed_all = lax.all_gather(single_normed, "row", axis=0, tiled=True)
    keys_all = jnp.dot(normed_all, w_key, preferred_element_type=jnp.float32).astype(jnp.bfloat16)
    values_all = jnp.dot(
        normed_all, w_value_gate[:, :channels], preferred_element_type=jnp.float32
    ).astype(jnp.bfloat16)
    query_heads = queries.reshape(row_count, head_count, head_size)
    key_heads = keys_all.reshape(length, head_count, head_size)
    value_heads = values_all.reshape(length, head_count, head_size)
    scores = (
        jnp.einsum("ihd,jhd->hij", query_heads, key_heads, preferred_element_type=jnp.float32)
        / jnp.sqrt(jnp.float32(head_size))
        + bias
    )
    scores = jnp.where(live_all[None, None, :] > 0, scores, jnp.float32(-1000000000.0))
    row_max = jnp.max(scores, axis=2, keepdims=True)
    weights = jnp.exp(scores - row_max)
    weights = weights / jnp.sum(weights, axis=2, keepdims=True)
    probs = weights.astype(jnp.bfloat16)
    attended = jnp.einsum(
        "hij,jhd->ihd", probs, value_heads, preferred_element_type=jnp.float32
    ).reshape(row_count, channels)
    gated = (att_gate * attended).astype(jnp.bfloat16)
    single_update = jnp.dot(gated, w_out, preferred_element_type=jnp.float32)
    return (pair_new, single_update)


def body(*arrays):
    pair, single, w_tri_out = arrays[0], arrays[1], arrays[5]
    row_count, length, _ = pair.shape
    groups = lax.axis_size("row")
    hidden = w_tri_out.shape[0]
    sets = groups // 2
    packs = (
        groups >= 4
        and groups & (groups - 1) == 0
        and hidden % (32 * sets) == 0
        and (length % LANES) * 2 == LANES
        and length // LANES == 1
        and row_count % SUB == 0
        and single.shape[1] % LANES == 0
        and all(groups * n * SUB in (LANES, LANES // 2) for n in chunk_tiles(row_count // SUB, groups))
        and bool(chunk_tiles(row_count // SUB, groups))
    )
    if not packs:
        return plain_body(*arrays)
    return fast_body(*arrays)


def solution(mesh):
    in_specs = (
        P(("crop", "row"), None, None),
        P(("crop", "row"), None),
        P("crop"),
        P(),
        P(),
        P(),
        P(),
        P(),
        P(),
        P(),
        P(),
        P(),
        P(),
    )
    out_specs = (P(("crop", "row"), None, None), P(("crop", "row"), None))
    return jax.shard_map(body, mesh=mesh, in_specs=in_specs, out_specs=out_specs, check_vma=False)
```

```python
import functools
import math

import jax
import jax.numpy as jnp
from jax import lax
from jax.experimental import pallas as pl
from jax.experimental.pallas import tpu as pltpu
from jax.sharding import PartitionSpec as P


epsilon = 1e-05
LANES = 128
SUB = 8
f32 = jnp.float32
bf16 = jnp.bfloat16
NT = (((1,), (1,)), ((), ()))


def layer_norm(values_in, along):
    average = jnp.mean(values_in, axis=along, keepdims=True)
    centered = values_in - average
    spread = jnp.mean(centered * centered, axis=along, keepdims=True)
    return centered * lax.rsqrt(spread + epsilon)


def sigmoid(x):
    return 0.5 * jnp.tanh(0.5 * x) + 0.5


def repeat_rest(x, full):
    return jnp.concatenate([x, x[full:]], axis=0)


def first_half_lanes(shape):
    return lax.broadcasted_iota(jnp.int32, shape, len(shape) - 1) < LANES // 2


def edges_to_messages(me_ref, mask_ref, live_ref, wt_ref, rows_of, head_ref, rest_ref, out_refs, first, hidden, full):
    sets = len(out_refs)
    per_set = hidden // sets
    pairs = per_set // 2
    stride = hidden + SUB
    own_set = lax.rem(me_ref[0], sets)
    tokens = live_ref[...].astype(f32).reshape(1, live_ref.shape[0])
    tokens = jnp.concatenate([tokens, tokens[:, full:]], axis=1)
    for j in range(SUB):
        x = repeat_rest(rows_of(j), full)
        projected = lax.dot_general(wt_ref[...], x, NT, preferred_element_type=f32)
        live = tokens * mask_ref[first + j].astype(f32)
        edge = sigmoid(projected[hidden:]) * projected[:hidden] * live
        for s in range(sets):
            q = lax.bitwise_xor(own_set, s)
            at = pl.multiple_of(j * stride + q * per_set, SUB)
            part = edge[s * per_set : (s + 1) * per_set]
            head_ref[pl.ds(at, per_set), :] = part[:, :LANES]
            rest_ref[pl.ds(at, per_set), :] = part[:, LANES:]
    step, tiles = pl.program_id(0), pl.num_programs(0)
    low = first_half_lanes((SUB, LANES))
    for q in range(sets):
        for c in range(pairs):
            a = pl.ds(q * per_set + c, SUB, stride=stride)
            b = pl.ds(q * per_set + pairs + c, SUB, stride=stride)
            out_refs[q][c * tiles + step] = head_ref[a, :].astype(bf16)
            out_refs[q][(pairs + c) * tiles + step] = head_ref[b, :].astype(bf16)
            out_refs[q][(per_set + c) * tiles + step] = jnp.where(low, rest_ref[a, :], rest_ref[b, :]).astype(bf16)


def right_kernel(hidden, full, sets, row_count, offset, single_tiles, me_ref, mask_ref, pair_ref, single_ref, live_ref, w_ref, *rest):
    out_refs = rest[-3 - sets : -3]
    head_ref, rest_ref, wt_ref = rest[-3:]

    @pl.when(pl.program_id(0) == 0)
    def _():
        wt_ref[...] = w_ref[...].T

    first = me_ref[0] * row_count + offset + pl.program_id(0) * SUB
    at = 0 if single_tiles else offset + pl.program_id(0) * SUB
    rows_of = lambda j: layer_norm(pair_ref[at + j], 1).astype(bf16)
    edges_to_messages(me_ref, mask_ref, live_ref, wt_ref, rows_of, head_ref, rest_ref, out_refs, first, hidden, full)
    if single_tiles:

        @pl.when(pl.program_id(0) == 0)
        def _():
            single_normed = layer_norm(single_ref[...], 1)
            base = hidden // sets * 3 // 2 * single_tiles
            for n in range(single_ref.shape[1] // LANES * (row_count // SUB)):
                t, at = divmod(n, row_count // SUB)
                part = single_normed[at * SUB : (at + 1) * SUB, t * LANES : (t + 1) * LANES].astype(bf16)
                for q in range(sets):
                    out_refs[q][base + n] = part


def left_kernel(hidden, full, sets, row_count, me_ref, mask_ref, pair_ref, live_ref, w_ref, *rest):
    out_refs = rest[-3 - sets : -3]
    head_ref, rest_ref, wt_ref = rest[-3:]

    @pl.when(pl.program_id(0) == 0)
    def _():
        wt_ref[...] = w_ref[...].T

    first = me_ref[0] * row_count + pl.program_id(0) * SUB
    rows_of = lambda j: layer_norm(pair_ref[pl.program_id(0) * SUB + j], 1).astype(bf16)
    edges_to_messages(me_ref, mask_ref, live_ref, wt_ref, rows_of, head_ref, rest_ref, out_refs, first, hidden, full)


def gate_kernel(pair_ref, w_gate_ref, _, gate_ref):
    width = pair_ref.shape[2]

    def rows(g, carry):
        here = pl.ds(g * SUB, SUB)
        block = pair_ref[here]
        x = layer_norm(block.reshape(SUB * block.shape[1], width), 1).astype(bf16)
        gate_ref[here] = sigmoid(jnp.dot(x, w_gate_ref[...], preferred_element_type=f32)).reshape(block.shape)
        return carry

    lax.fori_loop(0, pair_ref.shape[0] // SUB, rows, 0)


def plain_rows(block):
    wide = block.astype(f32)
    return wide.reshape(wide.shape[0] * wide.shape[1], wide.shape[2])


def triangle_kernel(groups, sets, per_set, here, me_ref, *refs):
    right_refs, left_refs = refs[:groups], refs[groups : groups + sets]
    out_refs = refs[-sets - 3 : -3]
    head_ref, rest_ref, sums_ref = refs[-3:]
    pairs = per_set // 2
    rows = left_refs[0].shape[0] // (per_set + pairs) * SUB
    columns = groups * here
    me = me_ref[0]
    total = sets * rows
    stride = total + SUB
    low = first_half_lanes((total, LANES))
    mine = lambda r, c: plain_rows(r[c * rows // SUB : (c + 1) * rows // SUB])
    fill = lambda x: x if columns == LANES else jnp.concatenate([x, x], axis=0)
    for s in range(groups):
        d = lax.bitwise_xor(me, s)
        wide = right_refs[s][: (per_set + pairs) * here // SUB].astype(f32).reshape(per_set + pairs, here, LANES)
        head_ref[:, d] = wide[:per_set]
        rest_ref[:, d] = wide[per_set:]
    for c in range(pairs):
        right_rest = fill(rest_ref[c].reshape(columns, LANES)).astype(bf16)
        left_rest = jnp.concatenate([mine(r, per_set + c) for r in left_refs], axis=0)
        for p in range(2):
            channel = p * pairs + c
            right = fill(head_ref[channel].reshape(columns, LANES)).astype(bf16)
            left = jnp.concatenate([mine(r, channel) for r in left_refs], axis=0).astype(bf16)
            kept = jnp.where(low if p == 0 else jnp.logical_not(low), left_rest, 0.0).astype(bf16)
            sums_ref[channel * stride : channel * stride + total, :] = lax.dot_general(
                jnp.concatenate([left, kept], axis=1),
                jnp.concatenate([right, right_rest], axis=1),
                NT,
                preferred_element_type=f32,
            )
    low_half = first_half_lanes((pairs, LANES))
    for a in range(sets):
        for i in range(rows):
            x = sums_ref[pl.ds(a * rows + i, per_set, stride=stride), :]
            if columns < LANES:
                x = jnp.where(low_half, x[:pairs], x[pairs:])
            out_refs[a][i] = x.astype(bf16)


def attention_in_kernel(groups, chunks, message, me_ref, *refs):
    count = len(chunks)
    right_refs = refs[:groups]
    w_query_ref, w_key_ref, w_value_gate_ref, q_ref, g_ref = refs[groups : groups + 5]
    k_refs, v_refs = refs[groups + 5 : groups + 5 + count], refs[groups + 5 + count : groups + 5 + 2 * count]
    all_ref = refs[-1]
    channels = w_query_ref.shape[0]
    me = me_ref[0]
    tiles = all_ref.shape[1] // SUB
    for s in range(groups):
        d = lax.bitwise_xor(me, s)
        for n in range(channels // LANES * tiles):
            t, at = divmod(n, tiles)
            all_ref[d, at * SUB : (at + 1) * SUB, t * LANES : (t + 1) * LANES] = right_refs[s][message + n].astype(f32)
    own = all_ref[me].astype(bf16)
    q_ref[...] = jnp.dot(own, w_query_ref[...], preferred_element_type=f32).astype(bf16)
    g_ref[...] = sigmoid(jnp.dot(own, w_value_gate_ref[:, channels:], preferred_element_type=f32))
    first = 0
    for k in range(count):
        every = all_ref[:, first * SUB : (first + chunks[k]) * SUB].reshape(k_refs[k].shape).astype(bf16)
        k_refs[k][...] = jnp.dot(every, w_key_ref[...], preferred_element_type=f32).astype(bf16)
        v_refs[k][...] = jnp.dot(every, w_value_gate_ref[:, :channels], preferred_element_type=f32).astype(bf16)
        first += chunks[k]


def tail_kernel(sets, per_set, heads, slab, attends, first, me_ref, *refs):
    tri_refs = refs[:sets]
    pair_ref, gate_ref, w_tri_out_ref, w_in_ref, w_down_ref, w_bias_ref = refs[sets : sets + 6]
    if attends:
        new_ref, single_ref, bias_ref, w_rel_ref, w_half_ref = refs[-5:]
    else:
        new_ref, bias_ref, w_rel_ref, w_half_ref = refs[-4:]
    width = pair_ref.shape[-1]
    columns = math.prod(new_ref.shape[1:-1])
    part = slice(first, first + new_ref.shape[2])
    together = LANES // columns
    inner_width = w_down_ref.shape[0]
    me = me_ref[0]

    @pl.when(pl.program_id(0) == 0)
    def _():
        own_set = lax.rem(me, sets)
        for a in range(sets):
            w_rel_ref[a * per_set : (a + 1) * per_set] = w_tri_out_ref[lax.bitwise_xor(own_set, a)]
        w_half_ref[:, :inner_width] = w_in_ref[:, :inner_width] * 0.5
        w_half_ref[:, inner_width:] = w_in_ref[:, inner_width:]

    low = first_half_lanes((per_set // 2, LANES))
    start = pl.program_id(0) * new_ref.shape[0]

    def sums_of(i):
        parts = []
        for r in tri_refs:
            if together == 1:
                parts.append(r[i].astype(f32))
            else:
                here, there = r[i].astype(f32), r[i + 1].astype(f32)
                parts.append(jnp.where(low, here, pltpu.roll(there, LANES // 2, 1)))
                parts.append(jnp.where(low, pltpu.roll(here, LANES // 2, 1), there))
        return jnp.concatenate(parts, axis=0)

    def rows(b, carry):
        i = b * slab * together
        tri = []
        for n in range(slab):
            tri.append(layer_norm(sums_of(start + i + n * together), 0).astype(bf16).T)
        tri = jnp.concatenate(tri, axis=0)
        tri_out = jnp.dot(tri, w_rel_ref[...], preferred_element_type=f32)
        here, there = pl.ds(i, slab * together), pl.ds(start + i, slab * together)
        block = (slab * LANES, width)
        mid = pair_ref[there, :, part].reshape(block) + gate_ref[there, :, part].reshape(block) * tri_out
        trans = layer_norm(mid, 1).astype(bf16)
        gate_up = jnp.dot(trans, w_half_ref[...], preferred_element_type=f32)
        half = gate_up[:, :inner_width]
        scaled = half * gate_up[:, inner_width:]
        inner = (scaled + scaled * jnp.tanh(half)).astype(bf16)
        new = mid + jnp.dot(inner, w_down_ref[...], preferred_element_type=f32)
        new_ref[here] = new.reshape((slab * together,) + new_ref.shape[1:])
        normed = layer_norm(new, 1).astype(bf16)
        bias = lax.dot_general(w_bias_ref[...], normed, NT, preferred_element_type=f32)
        for n in range(slab):
            lane_tile = bias[:, n * LANES : (n + 1) * LANES]
            bias_ref[i + n * together] = lane_tile
            if together == 2:
                bias_ref[i + n * together + 1] = pltpu.roll(lane_tile, LANES // 2, 1)
        return carry

    lax.fori_loop(0, new_ref.shape[0] // (slab * together), rows, 0)
    if attends:
        attention(heads, attends, pair_ref.shape[1], refs[sets + 6 :], bias_ref, single_ref)


def attention(heads, n, groups, refs, last_bias_ref, single_ref):
    q_ref, g_ref, w_out_ref, mask_ref = refs[:4]
    k_refs, v_refs = refs[4 : 4 + n], refs[4 + n : 4 + 2 * n]
    bias_refs = [*refs[4 + 2 * n : 3 + 3 * n], last_bias_ref]
    count = jnp.sum(mask_ref[...].astype(f32).reshape(1, mask_ref.shape[0]), axis=1, keepdims=True)
    row_count, channels = q_ref.shape
    head_size = channels // heads
    of_head = lax.broadcasted_iota(jnp.int32, (row_count, heads, channels), 1)
    lane = lax.broadcasted_iota(jnp.int32, (row_count, heads, channels), 2)
    mine = jnp.logical_and(lane >= of_head * head_size, lane < (of_head + 1) * head_size)
    spread = jnp.where(mine, jnp.broadcast_to(q_ref[...].astype(f32)[:, None, :], mine.shape), 0.0)
    spread = spread.reshape(row_count * heads, channels).astype(bf16)
    scores, first = [], 0
    for k in range(n):
        part = lax.dot_general(spread, k_refs[k][...], NT, preferred_element_type=f32)
        bias = bias_refs[k][...].reshape(row_count * heads, LANES)[:, : part.shape[1]]
        part = part / jnp.sqrt(f32(head_size)) + bias
        column = lax.broadcasted_iota(jnp.int32, (1, part.shape[1]), 1)
        size = part.shape[1] // groups
        token = column // size * row_count + first + column % size
        first += size
        scores.append(jnp.where(token.astype(f32) < count, part, f32(-1000000000.0)))
    row_max = functools.reduce(jnp.maximum, [jnp.max(x, axis=1, keepdims=True) for x in scores])
    weights = [jnp.exp(x - row_max) for x in scores]
    row_sum = sum(jnp.sum(x, axis=1, keepdims=True) for x in weights)
    attended = sum(
        jnp.dot((x / row_sum).astype(bf16), v[...], preferred_element_type=f32) for x, v in zip(weights, v_refs)
    )
    attended = jnp.sum(jnp.where(mine, attended.reshape(mine.shape), 0.0), axis=1)
    gated = (g_ref[...] * attended).astype(bf16)
    single_ref[...] = jnp.dot(gated, w_out_ref[...], preferred_element_type=f32)


def whole_block(shape):
    return pl.BlockSpec(shape, lambda *_: (0,) * len(shape))


def params(**more):
    return pltpu.CompilerParams(dimension_semantics=("arbitrary",), **more)


def arrived(arrays):
    return [pltpu.with_memory_space_constraint(x, pltpu.VMEM) for x in arrays]


def kept(arrays):
    return [pltpu.with_memory_space_constraint(x, pltpu.HBM) for x in arrays]


def in_vmem(arrays):
    return [pl.BlockSpec(memory_space=pltpu.VMEM)] * len(arrays)


def anywhere(arrays):
    return [pl.BlockSpec(memory_space=pl.ANY)] * len(arrays)


def cost(flops):
    return pl.CostEstimate(flops=int(flops), bytes_accessed=4000000, transcendentals=0)


def exchange(x, groups, s):
    return x if s == 0 else lax.ppermute(x, "row", [(r, r ^ s) for r in range(groups)])


def chunk_tiles(tiles, groups):
    most = LANES // (groups * SUB)
    chunks = [most] * (tiles // most) if most else []
    return chunks + ([tiles % most] if most and tiles % most else [])


def fast_body(
    pair, single, token_mask, w_tri_proj, w_tri_gate, w_tri_out, w_trans_in, w_trans_out, w_bias, w_query, w_key, w_value_gate, w_out
):
    row_count, length, width = pair.shape
    groups = lax.axis_size("row")
    sets = groups // 2
    hidden = w_tri_out.shape[0]
    per_set = hidden // sets
    message = per_set * 3 // 2
    inner_width = w_trans_out.shape[0]
    heads = w_bias.shape[1]
    channels = single.shape[1]
    full = length // LANES * LANES
    lanes = full + LANES
    tiles = row_count // SUB
    singles = channels // LANES * tiles
    chunks = chunk_tiles(tiles, groups)
    starts = [sum(chunks[:k]) for k in range(len(chunks))]
    me = lax.axis_index("row").astype(jnp.int32).reshape(1)
    (near,) = arrived([pair])
    sds = jax.ShapeDtypeStruct
    edge_scratch = [pltpu.VMEM((SUB * (hidden + SUB), LANES), f32)] * 2 + [pltpu.VMEM((2 * hidden, width), bf16)]
    edge_flops = 2 * SUB * lanes * width * 2 * hidden

    def right_edges(k, after):
        at = starts[k]
        size = message * chunks[k] + (0 if k else singles)
        return pl.pallas_call(
            functools.partial(right_kernel, hidden, full, sets, row_count, at * SUB, 0 if k else chunks[0]),
            name="right",
            grid_spec=pltpu.PrefetchScalarGridSpec(
                num_scalar_prefetch=2,
                grid=(chunks[k],),
                in_specs=[
                    *(in_vmem([near]) if k else [pl.BlockSpec((SUB, length, width), lambda g, *_: (g, 0, 0))]),
                    whole_block(single.shape),
                    whole_block((length,)),
                    pl.BlockSpec((width, 2 * hidden), lambda *_: (0, 1)),
                ]
                + anywhere(after),
                out_specs=in_vmem([None] * sets),
                scratch_shapes=edge_scratch,
            ),
            out_shape=[sds((size, SUB, LANES), bf16)] * sets,
            compiler_params=params(vmem_limit_bytes=24 * 2**20),
            cost_estimate=cost(edge_flops * chunks[k]),
        )(me, token_mask, *([near, single, token_mask, w_tri_proj] if k else kept([pair, single, token_mask, w_tri_proj])), *after)

    def left_edges(after):
        return pl.pallas_call(
            functools.partial(left_kernel, hidden, full, sets, row_count),
            name="left",
            grid_spec=pltpu.PrefetchScalarGridSpec(
                num_scalar_prefetch=2,
                grid=(tiles,),
                in_specs=[
                    *in_vmem([near]),
                    whole_block((length,)),
                    pl.BlockSpec((width, 2 * hidden), lambda *_: (0, 0)),
                ]
                + anywhere(after),
                out_specs=in_vmem([None] * sets),
                scratch_shapes=edge_scratch,
            ),
            out_shape=[sds((message * tiles, SUB, LANES), bf16)] * sets,
            compiler_params=params(vmem_limit_bytes=24 * 2**20),
            cost_estimate=cost(edge_flops * tiles),
        )(me, token_mask, near, token_mask, w_tri_proj, *after)

    right_in, left_in, after = [], None, []
    for k in range(len(chunks)):
        right = right_edges(k, after)
        right_in.append([exchange(right[s % sets], groups, s) for s in range(groups)])
        after = [right[0]]
        if left_in is None:
            left = left_edges(after)
            left_in = [exchange(left[s], groups, s) for s in range(sets)]
            after = [left[0]]

    gate_pair = pl.pallas_call(
        gate_kernel,
        name="gate",
        in_specs=in_vmem([near, w_tri_gate]) + anywhere(after),
        out_specs=in_vmem([None])[0],
        out_shape=sds(pair.shape, f32),
        compiler_params=pltpu.CompilerParams(vmem_limit_bytes=16 * 2**20),
        cost_estimate=cost(2 * row_count * length * width * width),
    )(near, w_tri_gate, *after)

    tokens = [groups * n * SUB for n in chunks]
    queries, att_gate, *keys_values = pl.pallas_call(
        functools.partial(attention_in_kernel, groups, chunks, message * chunks[0]),
        name="attention_in",
        grid_spec=pltpu.PrefetchScalarGridSpec(
            num_scalar_prefetch=1,
            grid=(1,),
            in_specs=in_vmem(right_in[0])
            + [whole_block(w_query.shape), whole_block(w_key.shape), whole_block(w_value_gate.shape)],
            out_specs=[whole_block((row_count, channels))] * 2 + [whole_block((n, channels)) for n in tokens + tokens],
            scratch_shapes=[pltpu.VMEM((groups, row_count, channels), f32)],
        ),
        out_shape=[sds((row_count, channels), bf16), sds((row_count, channels), f32)]
        + [sds((n, channels), bf16) for n in tokens + tokens],
        compiler_params=params(vmem_limit_bytes=16 * 2**20),
        cost_estimate=cost(2 * length * channels * channels * 3),
    )(me, *arrived(right_in[0]), w_query, w_key, w_value_gate)

    total = sets * row_count
    tri_in = []
    for k in range(len(chunks)):
        late = queries
        columns = groups * chunks[k] * SUB
        sums_shape = (row_count, per_set * columns // LANES, LANES)
        sums = pl.pallas_call(
            functools.partial(triangle_kernel, groups, sets, per_set, chunks[k] * SUB),
            grid_spec=pltpu.PrefetchScalarGridSpec(
                num_scalar_prefetch=1,
                grid=(1,),
                in_specs=in_vmem(right_in[k] + left_in) + anywhere([late]),
                out_specs=[whole_block(sums_shape)] * sets,
                scratch_shapes=[
                    pltpu.VMEM((per_set, groups, chunks[k] * SUB, LANES), f32),
                    pltpu.VMEM((per_set // 2, groups, chunks[k] * SUB, LANES), f32),
                    pltpu.VMEM((per_set * (total + SUB), LANES), f32),
                ],
            ),
            out_shape=[sds(sums_shape, bf16)] * sets,
            compiler_params=params(vmem_limit_bytes=24 * 2**20),
            cost_estimate=cost(2 * per_set * total * lanes * LANES),
        )(me, *arrived(right_in[k] + left_in), late)
        tri_in.append([exchange(sums[a], groups, a) for a in range(sets)])

    tiled = (row_count, groups, tiles, SUB, width)
    pair_tiled, gate_tiled = arrived([pair.reshape(tiled), gate_pair.reshape(tiled)])
    new, biases = None, []
    for k, n in enumerate(chunks):
        attends = len(chunks) if k == len(chunks) - 1 else 0
        columns = tokens[k]
        together = LANES // columns
        take = row_count
        slab = take // together
        at = starts[k] // n
        part_rows = pl.BlockSpec((take, groups, n, SUB, width), lambda g, *_, at=at: (g, 0, at, 0, 0))
        operands = [*arrived(tri_in[k]), pair_tiled, gate_tiled, w_tri_out.reshape(sets, per_set, width), w_trans_in, w_trans_out, w_bias.T]
        in_specs = in_vmem(operands[: sets + 2])
        if attends:
            operands += [queries, att_gate, w_out, token_mask, *keys_values, *biases]
        in_specs += [whole_block(x.shape) for x in operands[sets + 2 :]]
        aliases = {}
        if new is not None:
            aliases = {1 + len(operands): 0}
            operands.append(new)
            in_specs += anywhere([new])
        bias_shape = (row_count, heads, LANES)
        weights = [pltpu.VMEM((hidden, width), bf16), pltpu.VMEM(w_trans_in.shape, bf16)]
        new, last = pl.pallas_call(
            functools.partial(tail_kernel, sets, per_set, heads, slab, attends, starts[k]),
            grid_spec=pltpu.PrefetchScalarGridSpec(
                num_scalar_prefetch=1,
                grid=(row_count // take,),
                in_specs=in_specs,
                out_specs=[
                    part_rows,
                    whole_block(single.shape) if attends else pl.BlockSpec((take, heads, LANES), lambda g, *_: (g, 0, 0)),
                ],
                scratch_shapes=([pltpu.VMEM(bias_shape, f32)] if attends else []) + weights,
            ),
            out_shape=[sds(tiled, f32), sds(single.shape if attends else bias_shape, f32)],
            input_output_aliases=aliases,
            compiler_params=params(vmem_limit_bytes=32 * 2**20),
            cost_estimate=cost(2 * row_count * columns * width * (hidden + 3 * inner_width)),
        )(me, *operands)
        biases.append(last)
    return new.reshape(pair.shape), last


def triangle(pieces):
    left_op, right_op = pieces
    return jnp.einsum("gcik,gcjk->gcij", left_op, right_op, preferred_element_type=jnp.float32)


def plain_body(
    pair,
    single,
    token_mask,
    w_tri_proj,
    w_tri_gate,
    w_tri_out,
    w_trans_in,
    w_trans_out,
    w_bias,
    w_query,
    w_key,
    w_value_gate,
    w_out,
):
    row_count, length, pair_width = pair.shape
    groups = lax.axis_size("row")
    hidden = w_tri_out.shape[0]
    per_dev = hidden // groups
    inner_width = w_trans_out.shape[0]
    head_count = w_bias.shape[1]
    channels = single.shape[1]
    head_size = channels // head_count
    row_start = lax.axis_index("row") * row_count
    live_all = token_mask.astype(jnp.float32)
    own_live = lax.dynamic_slice_in_dim(live_all, row_start, row_count)
    pair_live = own_live[:, None] * live_all[None, :]
    normed = layer_norm(pair, 2).astype(jnp.bfloat16)

    def operand(offset):
        weights_two = w_tri_proj[:, offset * hidden : (offset + 2) * hidden].reshape(
            pair_width, 2, groups, per_dev
        )
        projected = jnp.einsum(
            "ikd,dsgc->sgcik", normed, weights_two, preferred_element_type=jnp.float32
        )
        return (jax.nn.sigmoid(projected[1]) * projected[0] * pair_live).astype(jnp.bfloat16)

    left_edge = operand(0)
    right_edge = operand(2)
    product = triangle(
        (
            lax.all_to_all(left_edge, "row", split_axis=0, concat_axis=2, tiled=True),
            lax.all_to_all(right_edge, "row", split_axis=0, concat_axis=2, tiled=True),
        )
    )
    returned = lax.all_to_all(
        product.astype(jnp.bfloat16), "row", split_axis=2, concat_axis=0, tiled=True
    ).astype(product.dtype)
    summed = returned.reshape(hidden, row_count, length)
    triangle_normed = layer_norm(summed, 0).astype(jnp.bfloat16)
    tri_out = jnp.einsum(
        "cij,cd->ijd", triangle_normed, w_tri_out, preferred_element_type=jnp.float32
    )
    gate_pair = jax.nn.sigmoid(
        jnp.einsum("ijc,cd->ijd", normed, w_tri_gate, preferred_element_type=jnp.float32)
    )
    pair_mid = pair + gate_pair * tri_out
    block_rows = math.gcd(row_count, 8)

    def transition(row_slab):
        trans_normed = layer_norm(row_slab, 2).astype(jnp.bfloat16)
        gate_up = jnp.einsum(
            "ijc,cf->ijf", trans_normed, w_trans_in, preferred_element_type=jnp.float32
        )
        inner_act = (jax.nn.silu(gate_up[..., :inner_width]) * gate_up[..., inner_width:]).astype(
            jnp.bfloat16
        )
        return row_slab + jnp.einsum(
            "ijf,fc->ijc", inner_act, w_trans_out, preferred_element_type=jnp.float32
        )

    pair_new = lax.map(
        transition, pair_mid.reshape(row_count // block_rows, block_rows, length, pair_width)
    ).reshape(row_count, length, pair_width)
    bias_normed = layer_norm(pair_new, 2).astype(jnp.bfloat16)
    bias = jnp.einsum("ijc,ch->hij", bias_normed, w_bias, preferred_element_type=jnp.float32)
    single_normed = layer_norm(single, 1).astype(jnp.bfloat16)
    queries = jnp.dot(single_normed, w_query, preferred_element_type=jnp.float32).astype(
        jnp.bfloat16
    )
    att_gate = jax.nn.sigmoid(
        jnp.dot(single_normed, w_value_gate[:, channels:], preferred_element_type=jnp.float32)
    )
    normed_all = lax.all_gather(single_normed, "row", axis=0, tiled=True)
    keys_all = jnp.dot(normed_all, w_key, preferred_element_type=jnp.float32).astype(jnp.bfloat16)
    values_all = jnp.dot(
        normed_all, w_value_gate[:, :channels], preferred_element_type=jnp.float32
    ).astype(jnp.bfloat16)
    query_heads = queries.reshape(row_count, head_count, head_size)
    key_heads = keys_all.reshape(length, head_count, head_size)
    value_heads = values_all.reshape(length, head_count, head_size)
    scores = (
        jnp.einsum("ihd,jhd->hij", query_heads, key_heads, preferred_element_type=jnp.float32)
        / jnp.sqrt(jnp.float32(head_size))
        + bias
    )
    scores = jnp.where(live_all[None, None, :] > 0, scores, jnp.float32(-1000000000.0))
    row_max = jnp.max(scores, axis=2, keepdims=True)
    weights = jnp.exp(scores - row_max)
    weights = weights / jnp.sum(weights, axis=2, keepdims=True)
    probs = weights.astype(jnp.bfloat16)
    attended = jnp.einsum(
        "hij,jhd->ihd", probs, value_heads, preferred_element_type=jnp.float32
    ).reshape(row_count, channels)
    gated = (att_gate * attended).astype(jnp.bfloat16)
    single_update = jnp.dot(gated, w_out, preferred_element_type=jnp.float32)
    return (pair_new, single_update)


def body(*arrays):
    pair, single, w_tri_out = arrays[0], arrays[1], arrays[5]
    row_count, length, _ = pair.shape
    groups = lax.axis_size("row")
    hidden = w_tri_out.shape[0]
    sets = groups // 2
    packs = (
        groups >= 4
        and groups & (groups - 1) == 0
        and hidden % (32 * sets) == 0
        and (length % LANES) * 2 == LANES
        and length // LANES == 1
        and row_count % SUB == 0
        and single.shape[1] % LANES == 0
        and all(groups * n * SUB in (LANES, LANES // 2) for n in chunk_tiles(row_count // SUB, groups))
        and bool(chunk_tiles(row_count // SUB, groups))
    )
    if not packs:
        return plain_body(*arrays)
    return fast_body(*arrays)


def solution(mesh):
    in_specs = (
        P(("crop", "row"), None, None),
        P(("crop", "row"), None),
        P("crop"),
        P(),
        P(),
        P(),
        P(),
        P(),
        P(),
        P(),
        P(),
        P(),
        P(),
    )
    out_specs = (P(("crop", "row"), None, None), P(("crop", "row"), None))
    return jax.shard_map(body, mesh=mesh, in_specs=in_specs, out_specs=out_specs, check_vma=False)
```

```python
import functools
import math

import jax
import jax.numpy as jnp
from jax import lax
from jax.experimental import pallas as pl
from jax.experimental.pallas import tpu as pltpu
from jax.sharding import PartitionSpec as P


epsilon = 1e-05
LANES = 128
SUB = 8
f32 = jnp.float32
bf16 = jnp.bfloat16
NT = (((1,), (1,)), ((), ()))


def layer_norm(values_in, along):
    average = jnp.mean(values_in, axis=along, keepdims=True)
    centered = values_in - average
    spread = jnp.mean(centered * centered, axis=along, keepdims=True)
    return centered * lax.rsqrt(spread + epsilon)


def sigmoid(x):
    return 0.5 * jnp.tanh(0.5 * x) + 0.5


def repeat_rest(x, full):
    return jnp.concatenate([x, x[full:]], axis=0)


def first_half_lanes(shape):
    return lax.broadcasted_iota(jnp.int32, shape, len(shape) - 1) < LANES // 2


def edges_to_messages(me_ref, mask_ref, live_ref, wt_ref, rows_of, head_ref, rest_ref, out_refs, first, hidden, full):
    sets = len(out_refs)
    per_set = hidden // sets
    pairs = per_set // 2
    stride = hidden + SUB
    own_set = lax.rem(me_ref[0], sets)
    tokens = live_ref[...].astype(f32).reshape(1, live_ref.shape[0])
    tokens = jnp.concatenate([tokens, tokens[:, full:]], axis=1)
    for j in range(SUB):
        x = repeat_rest(rows_of(j), full)
        projected = lax.dot_general(wt_ref[...], x, NT, preferred_element_type=f32)
        live = tokens * mask_ref[first + j].astype(f32)
        edge = sigmoid(projected[hidden:]) * projected[:hidden] * live
        for s in range(sets):
            q = lax.bitwise_xor(own_set, s)
            at = pl.multiple_of(j * stride + q * per_set, SUB)
            part = edge[s * per_set : (s + 1) * per_set]
            head_ref[pl.ds(at, per_set), :] = part[:, :LANES]
            rest_ref[pl.ds(at, per_set), :] = part[:, LANES:]
    step, tiles = pl.program_id(0), pl.num_programs(0)
    low = first_half_lanes((SUB, LANES))
    for q in range(sets):
        for c in range(pairs):
            a = pl.ds(q * per_set + c, SUB, stride=stride)
            b = pl.ds(q * per_set + pairs + c, SUB, stride=stride)
            out_refs[q][c * tiles + step] = head_ref[a, :].astype(bf16)
            out_refs[q][(pairs + c) * tiles + step] = head_ref[b, :].astype(bf16)
            out_refs[q][(per_set + c) * tiles + step] = jnp.where(low, rest_ref[a, :], rest_ref[b, :]).astype(bf16)


def right_kernel(hidden, full, sets, row_count, offset, single_tiles, me_ref, mask_ref, pair_ref, single_ref, live_ref, w_ref, *rest):
    out_refs = rest[-3 - sets : -3]
    head_ref, rest_ref, wt_ref = rest[-3:]

    @pl.when(pl.program_id(0) == 0)
    def _():
        wt_ref[...] = w_ref[...].T

    first = me_ref[0] * row_count + offset + pl.program_id(0) * SUB
    at = 0 if single_tiles else offset + pl.program_id(0) * SUB
    rows_of = lambda j: layer_norm(pair_ref[at + j], 1).astype(bf16)
    edges_to_messages(me_ref, mask_ref, live_ref, wt_ref, rows_of, head_ref, rest_ref, out_refs, first, hidden, full)
    if single_tiles:

        @pl.when(pl.program_id(0) == 0)
        def _():
            single_normed = layer_norm(single_ref[...], 1)
            base = hidden // sets * 3 // 2 * single_tiles
            for n in range(single_ref.shape[1] // LANES * (row_count // SUB)):
                t, at = divmod(n, row_count // SUB)
                part = single_normed[at * SUB : (at + 1) * SUB, t * LANES : (t + 1) * LANES].astype(bf16)
                for q in range(sets):
                    out_refs[q][base + n] = part


def left_kernel(hidden, full, sets, row_count, me_ref, mask_ref, pair_ref, live_ref, w_ref, *rest):
    out_refs = rest[-3 - sets : -3]
    head_ref, rest_ref, wt_ref = rest[-3:]

    @pl.when(pl.program_id(0) == 0)
    def _():
        wt_ref[...] = w_ref[...].T

    first = me_ref[0] * row_count + pl.program_id(0) * SUB
    rows_of = lambda j: layer_norm(pair_ref[pl.program_id(0) * SUB + j], 1).astype(bf16)
    edges_to_messages(me_ref, mask_ref, live_ref, wt_ref, rows_of, head_ref, rest_ref, out_refs, first, hidden, full)


def gate_kernel(pair_ref, w_gate_ref, _, gate_ref):
    width = pair_ref.shape[2]

    def rows(g, carry):
        here = pl.ds(g * SUB, SUB)
        block = pair_ref[here]
        x = layer_norm(block.reshape(SUB * block.shape[1], width), 1).astype(bf16)
        gate_ref[here] = sigmoid(jnp.dot(x, w_gate_ref[...], preferred_element_type=f32)).reshape(block.shape)
        return carry

    lax.fori_loop(0, pair_ref.shape[0] // SUB, rows, 0)


def plain_rows(block):
    wide = block.astype(f32)
    return wide.reshape(wide.shape[0] * wide.shape[1], wide.shape[2])


def triangle_kernel(groups, sets, per_set, here, me_ref, *refs):
    right_refs, left_refs = refs[:groups], refs[groups : groups + sets]
    out_refs = refs[-sets - 3 : -3]
    head_ref, rest_ref, sums_ref = refs[-3:]
    pairs = per_set // 2
    rows = left_refs[0].shape[0] // (per_set + pairs) * SUB
    columns = groups * here
    me = me_ref[0]
    total = sets * rows
    stride = total + SUB
    low = first_half_lanes((total, LANES))
    mine = lambda r, c: plain_rows(r[c * rows // SUB : (c + 1) * rows // SUB])
    fill = lambda x: x if columns == LANES else jnp.concatenate([x, x], axis=0)
    for s in range(groups):
        d = lax.bitwise_xor(me, s)
        wide = right_refs[s][: (per_set + pairs) * here // SUB].astype(f32).reshape(per_set + pairs, here, LANES)
        head_ref[:, d] = wide[:per_set]
        rest_ref[:, d] = wide[per_set:]
    for c in range(pairs):
        right_rest = fill(rest_ref[c].reshape(columns, LANES)).astype(bf16)
        left_rest = jnp.concatenate([mine(r, per_set + c) for r in left_refs], axis=0)
        for p in range(2):
            channel = p * pairs + c
            right = fill(head_ref[channel].reshape(columns, LANES)).astype(bf16)
            left = jnp.concatenate([mine(r, channel) for r in left_refs], axis=0).astype(bf16)
            kept = jnp.where(low if p == 0 else jnp.logical_not(low), left_rest, 0.0).astype(bf16)
            sums_ref[channel * stride : channel * stride + total, :] = lax.dot_general(
                jnp.concatenate([left, kept], axis=1),
                jnp.concatenate([right, right_rest], axis=1),
                NT,
                preferred_element_type=f32,
            )
    low_half = first_half_lanes((pairs, LANES))
    for a in range(sets):
        for i in range(rows):
            x = sums_ref[pl.ds(a * rows + i, per_set, stride=stride), :]
            if columns < LANES:
                x = jnp.where(low_half, x[:pairs], x[pairs:])
            out_refs[a][i] = x.astype(bf16)


def own_lanes(row_count, heads, channels):
    head_size = channels // heads
    of_head = lax.broadcasted_iota(jnp.int32, (row_count, heads, channels), 1)
    lane = lax.broadcasted_iota(jnp.int32, (row_count, heads, channels), 2)
    return jnp.logical_and(lane >= of_head * head_size, lane < (of_head + 1) * head_size)


def attention_in_kernel(groups, chunks, message, heads, me_ref, *refs):
    count = len(chunks)
    right_refs = refs[:groups]
    w_query_ref, w_key_ref, w_value_gate_ref, g_ref, late_ref = refs[groups : groups + 5]
    k_refs, v_refs = refs[groups + 5 : groups + 5 + count], refs[groups + 5 + count : groups + 5 + 2 * count]
    all_ref = refs[-1]
    channels = w_query_ref.shape[0]
    me = me_ref[0]
    tiles = all_ref.shape[1] // SUB
    for s in range(groups):
        d = lax.bitwise_xor(me, s)
        for n in range(channels // LANES * tiles):
            t, at = divmod(n, tiles)
            all_ref[d, at * SUB : (at + 1) * SUB, t * LANES : (t + 1) * LANES] = right_refs[s][message + n].astype(f32)
    own = all_ref[me].astype(bf16)
    queries = jnp.dot(own, w_query_ref[...], preferred_element_type=f32).astype(bf16)
    late_ref[...] = queries
    mine = own_lanes(own.shape[0], heads, channels)
    spread = jnp.where(mine, jnp.broadcast_to(queries.astype(f32)[:, None, :], mine.shape), 0.0)
    spread = spread.reshape(own.shape[0] * heads, channels).astype(bf16)
    g_ref[...] = sigmoid(jnp.dot(own, w_value_gate_ref[:, channels:], preferred_element_type=f32))
    first = 0
    for k in range(count):
        every = all_ref[:, first * SUB : (first + chunks[k]) * SUB].reshape(v_refs[k].shape).astype(bf16)
        keys = jnp.dot(every, w_key_ref[...], preferred_element_type=f32).astype(bf16)
        scores = lax.dot_general(spread, keys, NT, preferred_element_type=f32)
        k_refs[k][...] = scores / jnp.sqrt(f32(channels // heads))
        v_refs[k][...] = jnp.dot(every, w_value_gate_ref[:, :channels], preferred_element_type=f32).astype(bf16)
        first += chunks[k]


def tail_kernel(sets, per_set, heads, slab, attends, first, me_ref, *refs):
    tri_refs = refs[:sets]
    pair_ref, gate_ref, w_tri_out_ref, w_in_ref, w_down_ref, w_bias_ref = refs[sets : sets + 6]
    if attends:
        new_ref, single_ref, bias_ref, w_rel_ref, w_half_ref = refs[-5:]
    else:
        new_ref, bias_ref, w_rel_ref, w_half_ref = refs[-4:]
    width = pair_ref.shape[-1]
    columns = math.prod(new_ref.shape[1:-1])
    part = slice(first, first + new_ref.shape[2])
    together = LANES // columns
    inner_width = w_down_ref.shape[0]
    me = me_ref[0]

    @pl.when(pl.program_id(0) == 0)
    def _():
        own_set = lax.rem(me, sets)
        for a in range(sets):
            w_rel_ref[a * per_set : (a + 1) * per_set] = w_tri_out_ref[lax.bitwise_xor(own_set, a)]
        w_half_ref[:, :inner_width] = w_in_ref[:, :inner_width] * 0.5
        w_half_ref[:, inner_width:] = w_in_ref[:, inner_width:]

    low = first_half_lanes((per_set // 2, LANES))
    start = pl.program_id(0) * new_ref.shape[0]

    def sums_of(i):
        parts = []
        for r in tri_refs:
            if together == 1:
                parts.append(r[i].astype(f32))
            else:
                here, there = r[i].astype(f32), r[i + 1].astype(f32)
                parts.append(jnp.where(low, here, pltpu.roll(there, LANES // 2, 1)))
                parts.append(jnp.where(low, pltpu.roll(here, LANES // 2, 1), there))
        return jnp.concatenate(parts, axis=0)

    def rows(b, carry):
        i = b * slab * together
        tri = []
        for n in range(slab):
            tri.append(layer_norm(sums_of(start + i + n * together), 0).astype(bf16).T)
        tri = jnp.concatenate(tri, axis=0)
        tri_out = jnp.dot(tri, w_rel_ref[...], preferred_element_type=f32)
        here, there = pl.ds(i, slab * together), pl.ds(start + i, slab * together)
        block = (slab * LANES, width)
        mid = pair_ref[there, :, part].reshape(block) + gate_ref[there, :, part].reshape(block) * tri_out
        trans = layer_norm(mid, 1).astype(bf16)
        gate_up = jnp.dot(trans, w_half_ref[...], preferred_element_type=f32)
        half = gate_up[:, :inner_width]
        scaled = half * gate_up[:, inner_width:]
        inner = (scaled + scaled * jnp.tanh(half)).astype(bf16)
        new = mid + jnp.dot(inner, w_down_ref[...], preferred_element_type=f32)
        new_ref[here] = new.reshape((slab * together,) + new_ref.shape[1:])
        normed = layer_norm(new, 1).astype(bf16)
        bias = lax.dot_general(w_bias_ref[...], normed, NT, preferred_element_type=f32)
        for n in range(slab):
            lane_tile = bias[:, n * LANES : (n + 1) * LANES]
            bias_ref[i + n * together] = lane_tile
            if together == 2:
                bias_ref[i + n * together + 1] = pltpu.roll(lane_tile, LANES // 2, 1)
        return carry

    lax.fori_loop(0, new_ref.shape[0] // (slab * together), rows, 0)
    if attends:
        attention(heads, attends, pair_ref.shape[1], refs[sets + 6 :], bias_ref, single_ref)


def attention(heads, n, groups, refs, last_bias_ref, single_ref):
    g_ref, w_out_ref, mask_ref = refs[:3]
    score_refs, v_refs = refs[3 : 3 + n], refs[3 + n : 3 + 2 * n]
    bias_refs = [*refs[3 + 2 * n : 2 + 3 * n], last_bias_ref]
    count = jnp.sum(mask_ref[...].astype(f32).reshape(1, mask_ref.shape[0]), axis=1, keepdims=True)
    row_count, channels = g_ref.shape
    mine = own_lanes(row_count, heads, channels)
    scores, first = [], 0
    for k in range(n):
        part = score_refs[k][...]
        bias = bias_refs[k][...].reshape(row_count * heads, LANES)[:, : part.shape[1]]
        part = part + bias
        column = lax.broadcasted_iota(jnp.int32, (1, part.shape[1]), 1)
        size = part.shape[1] // groups
        token = column // size * row_count + first + column % size
        first += size
        scores.append(jnp.where(token.astype(f32) < count, part, f32(-1000000000.0)))
    row_max = functools.reduce(jnp.maximum, [jnp.max(x, axis=1, keepdims=True) for x in scores])
    weights = [jnp.exp(x - row_max) for x in scores]
    row_sum = sum(jnp.sum(x, axis=1, keepdims=True) for x in weights)
    attended = sum(
        jnp.dot((x / row_sum).astype(bf16), v[...], preferred_element_type=f32) for x, v in zip(weights, v_refs)
    )
    attended = jnp.sum(jnp.where(mine, attended.reshape(mine.shape), 0.0), axis=1)
    gated = (g_ref[...] * attended).astype(bf16)
    single_ref[...] = jnp.dot(gated, w_out_ref[...], preferred_element_type=f32)


def whole_block(shape):
    return pl.BlockSpec(shape, lambda *_: (0,) * len(shape))


def params(**more):
    return pltpu.CompilerParams(dimension_semantics=("arbitrary",), **more)


def arrived(arrays):
    return [pltpu.with_memory_space_constraint(x, pltpu.VMEM) for x in arrays]


def kept(arrays):
    return [pltpu.with_memory_space_constraint(x, pltpu.HBM) for x in arrays]


def in_vmem(arrays):
    return [pl.BlockSpec(memory_space=pltpu.VMEM)] * len(arrays)


def anywhere(arrays):
    return [pl.BlockSpec(memory_space=pl.ANY)] * len(arrays)


def cost(flops):
    return pl.CostEstimate(flops=int(flops), bytes_accessed=4000000, transcendentals=0)


def exchange(x, groups, s):
    return x if s == 0 else lax.ppermute(x, "row", [(r, r ^ s) for r in range(groups)])


def chunk_tiles(tiles, groups):
    most = LANES // (groups * SUB)
    chunks = [most] * (tiles // most) if most else []
    return chunks + ([tiles % most] if most and tiles % most else [])


def fast_body(
    pair, single, token_mask, w_tri_proj, w_tri_gate, w_tri_out, w_trans_in, w_trans_out, w_bias, w_query, w_key, w_value_gate, w_out
):
    row_count, length, width = pair.shape
    groups = lax.axis_size("row")
    sets = groups // 2
    hidden = w_tri_out.shape[0]
    per_set = hidden // sets
    message = per_set * 3 // 2
    inner_width = w_trans_out.shape[0]
    heads = w_bias.shape[1]
    channels = single.shape[1]
    full = length // LANES * LANES
    lanes = full + LANES
    tiles = row_count // SUB
    singles = channels // LANES * tiles
    chunks = chunk_tiles(tiles, groups)
    starts = [sum(chunks[:k]) for k in range(len(chunks))]
    me = lax.axis_index("row").astype(jnp.int32).reshape(1)
    (near,) = arrived([pair])
    sds = jax.ShapeDtypeStruct
    edge_scratch = [pltpu.VMEM((SUB * (hidden + SUB), LANES), f32)] * 2 + [pltpu.VMEM((2 * hidden, width), bf16)]
    edge_flops = 2 * SUB * lanes * width * 2 * hidden

    def right_edges(k, after):
        at = starts[k]
        size = message * chunks[k] + (0 if k else singles)
        return pl.pallas_call(
            functools.partial(right_kernel, hidden, full, sets, row_count, at * SUB, 0 if k else chunks[0]),
            name="right",
            grid_spec=pltpu.PrefetchScalarGridSpec(
                num_scalar_prefetch=2,
                grid=(chunks[k],),
                in_specs=[
                    *(in_vmem([near]) if k else [pl.BlockSpec((SUB, length, width), lambda g, *_: (g, 0, 0))]),
                    whole_block(single.shape),
                    whole_block((length,)),
                    pl.BlockSpec((width, 2 * hidden), lambda *_: (0, 1)),
                ]
                + anywhere(after),
                out_specs=in_vmem([None] * sets),
                scratch_shapes=edge_scratch,
            ),
            out_shape=[sds((size, SUB, LANES), bf16)] * sets,
            compiler_params=params(vmem_limit_bytes=24 * 2**20),
            cost_estimate=cost(edge_flops * chunks[k]),
        )(me, token_mask, *([near, single, token_mask, w_tri_proj] if k else kept([pair, single, token_mask, w_tri_proj])), *after)

    def left_edges(after):
        return pl.pallas_call(
            functools.partial(left_kernel, hidden, full, sets, row_count),
            name="left",
            grid_spec=pltpu.PrefetchScalarGridSpec(
                num_scalar_prefetch=2,
                grid=(tiles,),
                in_specs=[
                    *in_vmem([near]),
                    whole_block((length,)),
                    pl.BlockSpec((width, 2 * hidden), lambda *_: (0, 0)),
                ]
                + anywhere(after),
                out_specs=in_vmem([None] * sets),
                scratch_shapes=edge_scratch,
            ),
            out_shape=[sds((message * tiles, SUB, LANES), bf16)] * sets,
            compiler_params=params(vmem_limit_bytes=24 * 2**20),
            cost_estimate=cost(edge_flops * tiles),
        )(me, token_mask, near, token_mask, w_tri_proj, *after)

    right_in, left_in, after = [], None, []
    for k in range(len(chunks)):
        right = right_edges(k, after)
        right_in.append([exchange(right[s % sets], groups, s) for s in range(groups)])
        after = [right[0]]
        if left_in is None:
            left = left_edges(after)
            left_in = [exchange(left[s], groups, s) for s in range(sets)]
            after = [left[0]]

    gate_pair = pl.pallas_call(
        gate_kernel,
        name="gate",
        in_specs=in_vmem([near, w_tri_gate]) + anywhere(after),
        out_specs=in_vmem([None])[0],
        out_shape=sds(pair.shape, f32),
        compiler_params=pltpu.CompilerParams(vmem_limit_bytes=16 * 2**20),
        cost_estimate=cost(2 * row_count * length * width * width),
    )(near, w_tri_gate, *after)

    tokens = [groups * n * SUB for n in chunks]
    att_gate, queries, *keys_values = pl.pallas_call(
        functools.partial(attention_in_kernel, groups, chunks, message * chunks[0], heads),
        name="attention_in",
        grid_spec=pltpu.PrefetchScalarGridSpec(
            num_scalar_prefetch=1,
            grid=(1,),
            in_specs=in_vmem(right_in[0])
            + [whole_block(w_query.shape), whole_block(w_key.shape), whole_block(w_value_gate.shape)],
            out_specs=[whole_block((row_count, channels))] * 2
            + [whole_block((row_count * heads, n)) for n in tokens]
            + [whole_block((n, channels)) for n in tokens],
            scratch_shapes=[pltpu.VMEM((groups, row_count, channels), f32)],
        ),
        out_shape=[sds((row_count, channels), f32), sds((row_count, channels), bf16)]
        + [sds((row_count * heads, n), f32) for n in tokens]
        + [sds((n, channels), bf16) for n in tokens],
        compiler_params=params(vmem_limit_bytes=16 * 2**20),
        cost_estimate=cost(2 * length * channels * channels * 3),
    )(me, *arrived(right_in[0]), w_query, w_key, w_value_gate)

    total = sets * row_count
    tri_in = []
    for k in range(len(chunks)):
        late = queries
        columns = groups * chunks[k] * SUB
        sums_shape = (row_count, per_set * columns // LANES, LANES)
        sums = pl.pallas_call(
            functools.partial(triangle_kernel, groups, sets, per_set, chunks[k] * SUB),
            grid_spec=pltpu.PrefetchScalarGridSpec(
                num_scalar_prefetch=1,
                grid=(1,),
                in_specs=in_vmem(right_in[k] + left_in) + anywhere([late]),
                out_specs=[whole_block(sums_shape)] * sets,
                scratch_shapes=[
                    pltpu.VMEM((per_set, groups, chunks[k] * SUB, LANES), f32),
                    pltpu.VMEM((per_set // 2, groups, chunks[k] * SUB, LANES), f32),
                    pltpu.VMEM((per_set * (total + SUB), LANES), f32),
                ],
            ),
            out_shape=[sds(sums_shape, bf16)] * sets,
            compiler_params=params(vmem_limit_bytes=24 * 2**20),
            cost_estimate=cost(2 * per_set * total * lanes * LANES),
        )(me, *arrived(right_in[k] + left_in), late)
        tri_in.append([exchange(sums[a], groups, a) for a in range(sets)])

    tiled = (row_count, groups, tiles, SUB, width)
    pair_tiled, gate_tiled = arrived([pair.reshape(tiled), gate_pair.reshape(tiled)])
    new, biases = None, []
    for k, n in enumerate(chunks):
        attends = len(chunks) if k == len(chunks) - 1 else 0
        columns = tokens[k]
        together = LANES // columns
        take = row_count
        slab = take // together
        at = starts[k] // n
        part_rows = pl.BlockSpec((take, groups, n, SUB, width), lambda g, *_, at=at: (g, 0, at, 0, 0))
        operands = [*arrived(tri_in[k]), pair_tiled, gate_tiled, w_tri_out.reshape(sets, per_set, width), w_trans_in, w_trans_out, w_bias.T]
        in_specs = in_vmem(operands[: sets + 2])
        if attends:
            operands += [att_gate, w_out, token_mask, *keys_values, *biases]
        in_specs += [whole_block(x.shape) for x in operands[sets + 2 :]]
        aliases = {}
        if new is not None:
            aliases = {1 + len(operands): 0}
            operands.append(new)
            in_specs += anywhere([new])
        bias_shape = (row_count, heads, LANES)
        weights = [pltpu.VMEM((hidden, width), bf16), pltpu.VMEM(w_trans_in.shape, bf16)]
        new, last = pl.pallas_call(
            functools.partial(tail_kernel, sets, per_set, heads, slab, attends, starts[k]),
            grid_spec=pltpu.PrefetchScalarGridSpec(
                num_scalar_prefetch=1,
                grid=(row_count // take,),
                in_specs=in_specs,
                out_specs=[
                    part_rows,
                    whole_block(single.shape) if attends else pl.BlockSpec((take, heads, LANES), lambda g, *_: (g, 0, 0)),
                ],
                scratch_shapes=([pltpu.VMEM(bias_shape, f32)] if attends else []) + weights,
            ),
            out_shape=[sds(tiled, f32), sds(single.shape if attends else bias_shape, f32)],
            input_output_aliases=aliases,
            compiler_params=params(vmem_limit_bytes=32 * 2**20),
            cost_estimate=cost(2 * row_count * columns * width * (hidden + 3 * inner_width)),
        )(me, *operands)
        biases.append(last)
    return new.reshape(pair.shape), last


def triangle(pieces):
    left_op, right_op = pieces
    return jnp.einsum("gcik,gcjk->gcij", left_op, right_op, preferred_element_type=jnp.float32)


def plain_body(
    pair,
    single,
    token_mask,
    w_tri_proj,
    w_tri_gate,
    w_tri_out,
    w_trans_in,
    w_trans_out,
    w_bias,
    w_query,
    w_key,
    w_value_gate,
    w_out,
):
    row_count, length, pair_width = pair.shape
    groups = lax.axis_size("row")
    hidden = w_tri_out.shape[0]
    per_dev = hidden // groups
    inner_width = w_trans_out.shape[0]
    head_count = w_bias.shape[1]
    channels = single.shape[1]
    head_size = channels // head_count
    row_start = lax.axis_index("row") * row_count
    live_all = token_mask.astype(jnp.float32)
    own_live = lax.dynamic_slice_in_dim(live_all, row_start, row_count)
    pair_live = own_live[:, None] * live_all[None, :]
    normed = layer_norm(pair, 2).astype(jnp.bfloat16)

    def operand(offset):
        weights_two = w_tri_proj[:, offset * hidden : (offset + 2) * hidden].reshape(
            pair_width, 2, groups, per_dev
        )
        projected = jnp.einsum(
            "ikd,dsgc->sgcik", normed, weights_two, preferred_element_type=jnp.float32
        )
        return (jax.nn.sigmoid(projected[1]) * projected[0] * pair_live).astype(jnp.bfloat16)

    left_edge = operand(0)
    right_edge = operand(2)
    product = triangle(
        (
            lax.all_to_all(left_edge, "row", split_axis=0, concat_axis=2, tiled=True),
            lax.all_to_all(right_edge, "row", split_axis=0, concat_axis=2, tiled=True),
        )
    )
    returned = lax.all_to_all(
        product.astype(jnp.bfloat16), "row", split_axis=2, concat_axis=0, tiled=True
    ).astype(product.dtype)
    summed = returned.reshape(hidden, row_count, length)
    triangle_normed = layer_norm(summed, 0).astype(jnp.bfloat16)
    tri_out = jnp.einsum(
        "cij,cd->ijd", triangle_normed, w_tri_out, preferred_element_type=jnp.float32
    )
    gate_pair = jax.nn.sigmoid(
        jnp.einsum("ijc,cd->ijd", normed, w_tri_gate, preferred_element_type=jnp.float32)
    )
    pair_mid = pair + gate_pair * tri_out
    block_rows = math.gcd(row_count, 8)

    def transition(row_slab):
        trans_normed = layer_norm(row_slab, 2).astype(jnp.bfloat16)
        gate_up = jnp.einsum(
            "ijc,cf->ijf", trans_normed, w_trans_in, preferred_element_type=jnp.float32
        )
        inner_act = (jax.nn.silu(gate_up[..., :inner_width]) * gate_up[..., inner_width:]).astype(
            jnp.bfloat16
        )
        return row_slab + jnp.einsum(
            "ijf,fc->ijc", inner_act, w_trans_out, preferred_element_type=jnp.float32
        )

    pair_new = lax.map(
        transition, pair_mid.reshape(row_count // block_rows, block_rows, length, pair_width)
    ).reshape(row_count, length, pair_width)
    bias_normed = layer_norm(pair_new, 2).astype(jnp.bfloat16)
    bias = jnp.einsum("ijc,ch->hij", bias_normed, w_bias, preferred_element_type=jnp.float32)
    single_normed = layer_norm(single, 1).astype(jnp.bfloat16)
    queries = jnp.dot(single_normed, w_query, preferred_element_type=jnp.float32).astype(
        jnp.bfloat16
    )
    att_gate = jax.nn.sigmoid(
        jnp.dot(single_normed, w_value_gate[:, channels:], preferred_element_type=jnp.float32)
    )
    normed_all = lax.all_gather(single_normed, "row", axis=0, tiled=True)
    keys_all = jnp.dot(normed_all, w_key, preferred_element_type=jnp.float32).astype(jnp.bfloat16)
    values_all = jnp.dot(
        normed_all, w_value_gate[:, :channels], preferred_element_type=jnp.float32
    ).astype(jnp.bfloat16)
    query_heads = queries.reshape(row_count, head_count, head_size)
    key_heads = keys_all.reshape(length, head_count, head_size)
    value_heads = values_all.reshape(length, head_count, head_size)
    scores = (
        jnp.einsum("ihd,jhd->hij", query_heads, key_heads, preferred_element_type=jnp.float32)
        / jnp.sqrt(jnp.float32(head_size))
        + bias
    )
    scores = jnp.where(live_all[None, None, :] > 0, scores, jnp.float32(-1000000000.0))
    row_max = jnp.max(scores, axis=2, keepdims=True)
    weights = jnp.exp(scores - row_max)
    weights = weights / jnp.sum(weights, axis=2, keepdims=True)
    probs = weights.astype(jnp.bfloat16)
    attended = jnp.einsum(
        "hij,jhd->ihd", probs, value_heads, preferred_element_type=jnp.float32
    ).reshape(row_count, channels)
    gated = (att_gate * attended).astype(jnp.bfloat16)
    single_update = jnp.dot(gated, w_out, preferred_element_type=jnp.float32)
    return (pair_new, single_update)


def body(*arrays):
    pair, single, w_tri_out = arrays[0], arrays[1], arrays[5]
    row_count, length, _ = pair.shape
    groups = lax.axis_size("row")
    hidden = w_tri_out.shape[0]
    sets = groups // 2
    packs = (
        groups >= 4
        and groups & (groups - 1) == 0
        and hidden % (32 * sets) == 0
        and (length % LANES) * 2 == LANES
        and length // LANES == 1
        and row_count % SUB == 0
        and single.shape[1] % LANES == 0
        and all(groups * n * SUB in (LANES, LANES // 2) for n in chunk_tiles(row_count // SUB, groups))
        and bool(chunk_tiles(row_count // SUB, groups))
    )
    if not packs:
        return plain_body(*arrays)
    return fast_body(*arrays)


def solution(mesh):
    in_specs = (
        P(("crop", "row"), None, None),
        P(("crop", "row"), None),
        P("crop"),
        P(),
        P(),
        P(),
        P(),
        P(),
        P(),
        P(),
        P(),
        P(),
        P(),
    )
    out_specs = (P(("crop", "row"), None, None), P(("crop", "row"), None))
    return jax.shard_map(body, mesh=mesh, in_specs=in_specs, out_specs=out_specs, check_vma=False)
```
